8 devices in a mesh: data: 1 (over z), model: 2 (over y), stage: 4 (over x, core).
Axes of the slice: x: 2, y: 2, z: 1, core: 2. Of those that a mesh axis runs over, the one named last changes fastest.
Arguments:
- x_enc: bfloat16 [12, 768, 768], P(('data', 'stage'))
- enc_len: int32 [12], P(('data', 'stage'))
- y_dec: bfloat16 [12, 1024, 768], P(('data', 'stage'))
- enc_wqkv: bfloat16 [2, 768, 3, 768], P(None, None, None, 'model')
- enc_wo: bfloat16 [2, 768, 768], P(None, 'model')
- enc_w1: bfloat16 [2, 768, 3072], P(None, None, 'model')
- enc_w2: bfloat16 [2, 3072, 768], P(None, 'model')
- enc_norm: float32 [2, 2, 768], replicated
- enc_final: float32 [768], replicated
- dec_wqkv: bfloat16 [2, 768, 3, 768], P(None, None, None, 'model')
- dec_wo: bfloat16 [2, 768, 768], P(None, 'model')
- crs_wq: bfloat16 [2, 768, 768], P(None, None, 'model')
- crs_wkv: bfloat16 [2, 768, 2, 768], P(None, None, None, 'model')
- crs_wo: bfloat16 [2, 768, 768], P(None, 'model')
- dec_w1: bfloat16 [2, 768, 3072], P(None, None, 'model')
- dec_w2: bfloat16 [2, 3072, 768], P(None, 'model')
- dec_norm: float32 [2, 3, 768], replicated
Outputs:
- output: bfloat16 [12, 1024, 768], P(('data', 'stage'))
All inputs are finite; a program needn't handle non-finite values.
Results may differ from the reference program's by a relative error of at most 0.0114763.
Values are sent between devices in bfloat16 or wider.
A program may use at most 1 GiB of HBM per device.

```python
import jax
import jax.numpy as jnp
from jax import lax

BATCH_ROWS = 12
SRC_LEN = 768
TGT_LEN = 1024
D_MODEL = 768
NUM_HEADS = 12
FF_DIM = 3072
ENC_LAYERS = 2
DEC_LAYERS = 2
HEAD_DIM = D_MODEL // NUM_HEADS
NORM_EPS = 1e-6
NEG_BIG = -1e30


def smooth_seq(key, num_rows, seq_len):
    key_a, key_b, key_c = jax.random.split(key, 3)
    walk_steps = jax.random.normal(key_a, (num_rows, seq_len, D_MODEL), jnp.float32)
    walk_sum = jnp.cumsum(walk_steps, axis=1) * (seq_len ** -0.5)
    start_vec = 0.6 * jax.random.normal(key_b, (num_rows, 1, D_MODEL), jnp.float32)
    noise_part = 0.7 * jax.random.normal(key_c, (num_rows, seq_len, D_MODEL), jnp.float32)
    return (walk_sum + start_vec + noise_part).astype(jnp.bfloat16)


def draw_lengths(key):
    key_a, key_b, key_c = jax.random.split(key, 3)
    low_len = SRC_LEN // 4
    lengths = jax.random.randint(key_a, (BATCH_ROWS,), low_len, SRC_LEN + 1, dtype=jnp.int32)
    top_pos = jax.random.randint(key_b, (), 0, BATCH_ROWS, dtype=jnp.int32)
    low_pos = (top_pos + 1 + jax.random.randint(key_c, (), 0, BATCH_ROWS - 1, dtype=jnp.int32)) % BATCH_ROWS
    row_idx = jnp.arange(BATCH_ROWS, dtype=jnp.int32)
    lengths = jnp.where(row_idx == top_pos, SRC_LEN, lengths)
    lengths = jnp.where(row_idx == low_pos, low_len, lengths)
    return lengths.astype(jnp.int32)


def normal_weight(key, shape, fan_in):
    return (jax.random.normal(key, shape, jnp.float32) * (fan_in ** -0.5)).astype(jnp.bfloat16)


def norm_gains(key, shape):
    return 1.0 + 0.25 * jax.random.normal(key, shape, jnp.float32)


def setup_inputs(seed: int = 0, part: int = 0) -> dict:
    data_key = jax.random.fold_in(jax.random.key(seed), part)
    key_x, key_len, key_y = jax.random.split(data_key, 3)
    weight_keys = jax.random.split(jax.random.key(seed + 1), 14)
    enc_shape = (ENC_LAYERS, D_MODEL, D_MODEL)
    dec_shape = (DEC_LAYERS, D_MODEL, D_MODEL)
    return {
        'x_enc': smooth_seq(key_x, BATCH_ROWS, SRC_LEN),
        'enc_len': draw_lengths(key_len),
        'y_dec': smooth_seq(key_y, BATCH_ROWS, TGT_LEN),
        'enc_wqkv': normal_weight(weight_keys[0], (ENC_LAYERS, D_MODEL, 3, D_MODEL), D_MODEL),
        'enc_wo': normal_weight(weight_keys[1], enc_shape, D_MODEL),
        'enc_w1': normal_weight(weight_keys[2], (ENC_LAYERS, D_MODEL, FF_DIM), D_MODEL),
        'enc_w2': normal_weight(weight_keys[3], (ENC_LAYERS, FF_DIM, D_MODEL), FF_DIM),
        'enc_norm': norm_gains(weight_keys[4], (ENC_LAYERS, 2, D_MODEL)),
        'enc_final': norm_gains(weight_keys[5], (D_MODEL,)),
        'dec_wqkv': normal_weight(weight_keys[6], (DEC_LAYERS, D_MODEL, 3, D_MODEL), D_MODEL),
        'dec_wo': normal_weight(weight_keys[7], dec_shape, D_MODEL),
        'crs_wq': normal_weight(weight_keys[8], dec_shape, D_MODEL),
        'crs_wkv': normal_weight(weight_keys[9], (DEC_LAYERS, D_MODEL, 2, D_MODEL), D_MODEL),
        'crs_wo': normal_weight(weight_keys[10], dec_shape, D_MODEL),
        'dec_w1': normal_weight(weight_keys[11], (DEC_LAYERS, D_MODEL, FF_DIM), D_MODEL),
        'dec_w2': normal_weight(weight_keys[12], (DEC_LAYERS, FF_DIM, D_MODEL), FF_DIM),
        'dec_norm': norm_gains(weight_keys[13], (DEC_LAYERS, 3, D_MODEL)),
    }


def matmul_f32(left, right):
    return jnp.dot(left, right, preferred_element_type=jnp.float32)


def add_residual(hidden, update):
    return (hidden.astype(jnp.float32) + update).astype(jnp.bfloat16)


def rms_norm(hidden, norm_gain):
    h_float = hidden.astype(jnp.float32)
    inv_rms = lax.rsqrt(jnp.mean(h_float * h_float, axis=-1, keepdims=True) + NORM_EPS)
    return (h_float * inv_rms * norm_gain).astype(jnp.bfloat16)


def attend(q_heads, k_heads, v_heads, att_mask):
    scores = jnp.einsum('qhd,khd->hqk', q_heads.astype(jnp.float32), k_heads.astype(jnp.float32)) * (HEAD_DIM ** -0.5)
    scores = jnp.where(att_mask[None], scores, NEG_BIG)
    attn_probs = jax.nn.softmax(scores, axis=-1).astype(jnp.bfloat16)
    context = jnp.einsum('hqk,khd->qhd', attn_probs.astype(jnp.float32), v_heads.astype(jnp.float32))
    return context.astype(jnp.bfloat16).reshape(q_heads.shape[0], D_MODEL)


def ffn_block(hidden, w_up, w_down, norm_gain):
    normed = rms_norm(hidden, norm_gain)
    up_act = jax.nn.gelu(matmul_f32(normed, w_up), approximate=True).astype(jnp.bfloat16)
    return add_residual(hidden, matmul_f32(up_act, w_down))


def self_block(hidden, w_qkv, w_out, norm_gain, att_mask):
    seq_len = hidden.shape[0]
    normed = rms_norm(hidden, norm_gain)
    qkv_heads = matmul_f32(normed, w_qkv.reshape(D_MODEL, 3 * D_MODEL)).astype(jnp.bfloat16).reshape(seq_len, 3, NUM_HEADS, HEAD_DIM)
    context = attend(qkv_heads[:, 0], qkv_heads[:, 1], qkv_heads[:, 2], att_mask)
    return add_residual(hidden, matmul_f32(context, w_out))


def encode_row(x_row, src_length, enc_weights, enc_final):
    key_ok = jnp.broadcast_to(jnp.arange(SRC_LEN)[None, :] < src_length, (SRC_LEN, SRC_LEN))

    def layer_step(hidden, layer_w):
        w_qkv, w_out, w_up, w_down, layer_gains = layer_w
        hidden = self_block(hidden, w_qkv, w_out, layer_gains[0], key_ok)
        hidden = ffn_block(hidden, w_up, w_down, layer_gains[1])
        return hidden, None

    final_hidden = lax.scan(layer_step, x_row, enc_weights)[0]
    return rms_norm(final_hidden, enc_final)


def decode_row(y_row, src_hidden, src_length, dec_weights):
    causal = jnp.arange(TGT_LEN)[:, None] >= jnp.arange(TGT_LEN)[None, :]
    cross_ok = jnp.broadcast_to(jnp.arange(SRC_LEN)[None, :] < src_length, (TGT_LEN, SRC_LEN))

    def layer_step(hidden, layer_w):
        w_qkv, w_out, cross_q, cross_kv, cross_out, w_up, w_down, layer_gains = layer_w
        hidden = self_block(hidden, w_qkv, w_out, layer_gains[0], causal)
        normed = rms_norm(hidden, layer_gains[1])
        q_heads = matmul_f32(normed, cross_q).astype(jnp.bfloat16).reshape(TGT_LEN, NUM_HEADS, HEAD_DIM)
        kv_heads = matmul_f32(src_hidden, cross_kv.reshape(D_MODEL, 2 * D_MODEL)).astype(jnp.bfloat16).reshape(SRC_LEN, 2, NUM_HEADS, HEAD_DIM)
        context = attend(q_heads, kv_heads[:, 0], kv_heads[:, 1], cross_ok)
        hidden = add_residual(hidden, matmul_f32(context, cross_out))
        hidden = ffn_block(hidden, w_up, w_down, layer_gains[2])
        return hidden, None

    return lax.scan(layer_step, y_row, dec_weights)[0]


def reference(x_enc, enc_len, y_dec, enc_wqkv, enc_wo, enc_w1, enc_w2, enc_norm, enc_final,
              dec_wqkv, dec_wo, crs_wq, crs_wkv, crs_wo, dec_w1, dec_w2, dec_norm):
    enc_weights = (enc_wqkv, enc_wo, enc_w1, enc_w2, enc_norm)
    dec_weights = (dec_wqkv, dec_wo, crs_wq, crs_wkv, crs_wo, dec_w1, dec_w2, dec_norm)
    src_hidden = lax.map(lambda row_items: encode_row(row_items[0], row_items[1], enc_weights, enc_final), (x_enc, enc_len))
    half_rows = BATCH_ROWS // 2
    paired_hidden = jnp.roll(src_hidden, -half_rows, axis=0)
    paired_len = jnp.roll(enc_len, -half_rows, axis=0)
    return lax.map(lambda row_items: decode_row(row_items[0], row_items[1], row_items[2], dec_weights), (y_dec, paired_hidden, paired_len))
```

```python
import functools
import math

import jax
import jax.numpy as jnp
from jax import lax
from jax.experimental import pallas as pl
from jax.experimental.pallas import tpu as pltpu
from jax.sharding import PartitionSpec as P


D = 768
HALF = 384
FF = 3072
NORM_EPS = 1e-6
NEG_BIG = -1e30
EXP_SCALE = 0.125 * math.log2(math.e)
GELU_C = math.sqrt(2.0 / math.pi)
PIECE_XOR = (0, 2, 1, 3)
QROWS = 192
OROWS = 96
TILE = 256
CHUNK = 256
LANES = 128
SUB = 16
HEAD_DIM = 64
VMEM_LIMIT = 60 * 1024 * 1024


def norm_rows(h, gain):
    hf = h.astype(jnp.float32)
    inv = lax.rsqrt(jnp.mean(hf * hf, axis=-1, keepdims=True) + NORM_EPS)
    return (hf * inv * gain).astype(jnp.bfloat16)


def gelu(x):
    return x * (0.5 + 0.5 * jnp.tanh(GELU_C * (x + 0.044715 * (x * x * x))))


def dot(a, b):
    return jnp.dot(a, b, preferred_element_type=jnp.float32)


def dot_t(a, b):
    return lax.dot_general(a, b, (((1,), (1,)), ((), ())), preferred_element_type=jnp.float32)


def runs_of(chunks):
    runs = []
    for c in chunks:
        if runs and runs[-1][0] + runs[-1][1] == c:
            runs[-1] = (runs[-1][0], runs[-1][1] + 1)
        else:
            runs.append((c, 1))
    return runs


def attn_weight_copies(stage, own, pieces, base, halves, w_s, wo_s, sems):
    ncol = HALF * len(halves)
    off = ncol - HALF
    qkv, out = [], []
    if own:
        for c, src in enumerate(own[:-1]):
            qkv.append(pltpu.make_async_copy(src, w_s.at[:, pl.ds(c * ncol, HALF)], sems[0]))
        out.append(pltpu.make_async_copy(own[-1], wo_s.at[pl.ds(0, HALF), :], sems[1]))
    for piece, mask in zip(pieces, PIECE_XOR):
        quarter = stage ^ mask
        r0 = pl.multiple_of(quarter * QROWS, QROWS)
        for c in range(3):
            qkv.append(pltpu.make_async_copy(piece.at[pl.ds(base + c * QROWS, QROWS), :],
                                             w_s.at[pl.ds(r0, QROWS), pl.ds(c * ncol + off, HALF)], sems[0]))
        r1 = pl.multiple_of(off + quarter * OROWS, OROWS)
        for c in range(2):
            out.append(pltpu.make_async_copy(piece.at[pl.ds(base + 3 * QROWS + c * OROWS, OROWS), :],
                                             wo_s.at[pl.ds(r1, OROWS), pl.ds(c * HALF, HALF)], sems[1]))
    return qkv, out


def ff_weight_copies(layer, stage, w1_ref, w2_ref, up_pieces, down_pieces, down_base, w1_s, w2_s, sems):
    hf = FF // 2
    own_up = [pltpu.make_async_copy(w1_ref.at[layer], w1_s.at[:, pl.ds(0, hf)], sems[0])]
    own_down = [pltpu.make_async_copy(w2_ref.at[layer], w2_s.at[pl.ds(0, hf), :], sems[1])]
    up, down = [], []
    for i, mask in enumerate(PIECE_XOR):
        quarter = stage ^ mask
        r0 = pl.multiple_of(quarter * QROWS, QROWS)
        for c in range(4):
            up.append(pltpu.make_async_copy(up_pieces[i].at[pl.ds(c * QROWS, QROWS), :],
                                            w1_s.at[pl.ds(r0, QROWS), pl.ds(hf + c * HALF, HALF)], sems[2]))
        r1 = pl.multiple_of(hf + quarter * HALF, HALF)
        for c in range(2):
            down.append(pltpu.make_async_copy(down_pieces[i].at[pl.ds(down_base + c * HALF, HALF), :],
                                              w2_s.at[pl.ds(r1, HALF), pl.ds(c * HALF, HALF)], sems[3]))
    return [own_up, own_down, up, down]


def start_all(copies):
    for copy in copies:
        copy.start()


def wait_all(copies):
    for copy in copies:
        copy.wait()


def ff_rows(h1, gain, w1_s, w2_s, waits=None):
    xn = norm_rows(h1, gain)
    acc = None
    for c in range(FF // D):
        cols = slice(c * D, (c + 1) * D)
        second = c * D >= FF // 2
        if waits is not None and c in (0, FF // D // 2):
            wait_all(waits[2 * second])
        act = gelu(dot(xn, w1_s[:, cols])).astype(jnp.bfloat16)
        if waits is not None and c in (0, FF // D // 2):
            wait_all(waits[2 * second + 1])
        term = dot(act, w2_s[cols, :])
        acc = term if acc is None else acc + term
    return (h1.astype(jnp.float32) + acc).astype(jnp.bfloat16)


def pack_kernel(cfg, *refs):
    ins, outs, sem = refs[:cfg['nin']], refs[cfg['nin']:-1], refs[-1]
    stage = lax.axis_index('stage')
    copies = []
    for out, parts in zip(outs, cfg['groups']):
        base = 0
        for slot, index in parts:
            ref = ins[slot]
            size = ref.shape[-2] // 4
            for c in range(ref.shape[-1] // HALF):
                src = ref.at[index + (pl.ds(pl.multiple_of(stage * size, size), size), pl.ds(c * HALF, HALF))]
                copies.append(pltpu.make_async_copy(src, out.at[pl.ds(base, size), :], sem))
                base += size
    start_all(copies)
    wait_all(copies)


def group_rows(sources, parts):
    return sum(sources[slot].shape[-2] * sources[slot].shape[-1] // (4 * HALF) for slot, _ in parts)


def run_pack(sources, groups):
    hbm = pl.BlockSpec(memory_space=pl.ANY)
    vm = pl.BlockSpec(memory_space=pltpu.VMEM)
    shapes = [jax.ShapeDtypeStruct((group_rows(sources, parts), HALF), jnp.bfloat16) for parts in groups]
    return pl.pallas_call(
        functools.partial(pack_kernel, dict(nin=len(sources), groups=groups)),
        out_shape=shapes,
        in_specs=[hbm] * len(sources),
        out_specs=[vm] * len(groups),
        scratch_shapes=[pltpu.SemaphoreType.DMA],
        compiler_params=pltpu.CompilerParams(vmem_limit_bytes=VMEM_LIMIT),
        cost_estimate=pl.CostEstimate(flops=0, bytes_accessed=sum(4 * shape.size for shape in shapes), transcendentals=0),
    )(*sources)


def rows_at(i, size):
    return pl.ds(pl.multiple_of(i * size, size), size)


def project(h_ref, gain, w_s, cols, first, count, tile, dests, npair):
    def body(i, carry):
        rows = rows_at(first // tile + i, tile)
        x = h_ref[rows, :] if gain is None else norm_rows(h_ref[rows, :], gain)
        value = dot(x, w_s[:, cols])
        for d, dst in enumerate(dests):
            for pair in range(npair):
                col = (d * npair + pair) * LANES
                dst[pair, rows, :] = value[:, col:col + LANES].astype(jnp.bfloat16)
        return carry

    lax.fori_loop(0, count // tile, body, 0)


def attention(job, pairs, src_len, off_a, off_b, model_idx, q_s, k_s, v_s, km_s, vx_s, ctx_s):
    tq, tk, chunk_plan = job['tq'], job['tk'], job['chunks']
    causal = chunk_plan is not None
    qb = LANES
    npair = pairs
    lane = lax.broadcasted_iota(jnp.int32, (1, LANES), 1)
    lo_f = jnp.where(lane < HEAD_DIM, 1.0, 0.0).astype(jnp.float32)
    masks_f = (lo_f, 1.0 - lo_f)
    masks_b = [mask.astype(jnp.bfloat16) for mask in masks_f]
    nchunk = tk // CHUNK

    def pair_body(pair, carry):
        if not causal:
            k_first = jnp.where(off_a == 0, k_s[pair, 0:SUB, :].astype(jnp.float32)[0:1],
                                k_s[pair, HALF:HALF + SUB, :].astype(jnp.float32)[0:1])
        for c in range(nchunk):
            rows = slice(c * CHUNK, (c + 1) * CHUNK)
            v_f = v_s[pair, rows, :].astype(jnp.float32)
            ones = jnp.ones((CHUNK, LANES), jnp.float32)
            if not causal:
                idx = lax.broadcasted_iota(jnp.int32, (CHUNK, LANES), 0) + c * CHUNK
                pos = jnp.where(idx < HALF, idx + off_a, idx + (off_b - HALF))
                ok = pos < src_len
                km_s[rows, :] = jnp.where(ok, k_s[pair, rows, :].astype(jnp.float32), k_first).astype(jnp.bfloat16)
                v_f = jnp.where(ok, v_f, 0.0)
                ones = jnp.where(ok, ones, 0.0)
            for head, mask in enumerate(masks_f):
                vrows = slice((2 * c + head) * CHUNK, (2 * c + head + 1) * CHUNK)
                vx_s[vrows, :LANES] = (v_f * mask).astype(jnp.bfloat16)
                vx_s[vrows, LANES:] = (ones * mask).astype(jnp.bfloat16)
        for b in range(tq // qb):
            rows = slice(b * qb, (b + 1) * qb)
            qp = q_s[pair, rows, :]
            q2 = jnp.concatenate([qp * mask for mask in masks_b], axis=0)
            chunks, masks = chunk_plan[b * qb // CHUNK] if causal else (list(range(nchunk)), {})
            parts = []
            for start, count in runs_of(chunks):
                krows = slice(start * CHUNK, (start + count) * CHUNK)
                s_run = dot_t(q2, k_s[pair, krows, :] if causal else km_s[krows, :])
                for j in range(count):
                    s_c = s_run[:, j * CHUNK:(j + 1) * CHUNK]
                    kind = masks.get(start + j)
                    if kind == 'diag':
                        q_idx = lax.broadcasted_iota(jnp.int32, (2 * qb, CHUNK), 0)
                        q_idx = jnp.where(q_idx < qb, q_idx, q_idx - qb) + (b * qb % CHUNK)
                        k_idx = lax.broadcasted_iota(jnp.int32, (2 * qb, CHUNK), 1)
                        s_c = jnp.where(k_idx <= q_idx, s_c, NEG_BIG)
                    elif kind is not None:
                        s_c = jnp.where(model_idx == kind, s_c, NEG_BIG)
                    parts.append(s_c)
            top = functools.reduce(jnp.maximum, parts)
            top = jnp.max(top, axis=-1, keepdims=True)
            probs = [jnp.exp2((part - top) * EXP_SCALE).astype(jnp.bfloat16) for part in parts]
            terms = []
            for start, count in runs_of(chunks):
                used, probs = probs[:count], probs[count:]
                lhs = [half for prob in used for half in (prob[:qb], prob[qb:])]
                terms.append(dot(jnp.concatenate(lhs, axis=1), vx_s[2 * start * CHUNK:2 * (start + count) * CHUNK, :]))
            total = functools.reduce(jnp.add, terms)
            ctx_s[pair, rows, :] = (total[:, :LANES] / total[:, LANES:]).astype(jnp.bfloat16)
        return carry

    lax.fori_loop(0, npair, pair_body, 0)


def block_kernel(cfg, *refs):
    it = iter(refs)

    def take(n):
        return [next(it) for _ in range(n)]

    layer, kind, halves, ff, jobs = cfg['layer'], cfg['kind'], cfg['halves'], cfg['ff'], cfg['jobs']
    cross = kind == 'cross'
    nh = len(halves)
    npair, ncol = 3 * nh, HALF * nh
    lens, norm_ref = take(2)
    final_ref = take(1)[0] if cfg['final'] else None
    data = take(cfg['ndata'])
    own_refs = take(cfg['nown'])
    pieces = take(cfg['npiece'])
    if ff:
        w1_ref, w2_ref = take(2)
        up_pieces, down_pieces = take(4), take(4)
    outs = take(len(jobs))
    h_bufs = take(len(jobs))
    s_bufs = take(len(jobs)) if cross else None
    p_bufs = take(len(jobs)) if cfg['part_in'] else None
    o_bufs = take(len(jobs))
    if kind:
        w_s, wo_s, q_s, k_s, v_s, km_s, vx_s, ctx_s = take(8)
    if ff:
        w1_s, w2_s = take(2)
    sem, job_sem, out_sem = take(3)
    m, stage = lax.axis_index('model'), lax.axis_index('stage')

    def load(parts, dst, semaphore):
        copies, base = [], 0
        for slot, lead, size, steps in parts:
            for a, b in steps:
                start = pl.multiple_of((a + b * m) * size, size) if lead is not None else 0
                index = (pl.ds(start, size), slice(None))
                if lead is not None:
                    index = (lead[0] + lead[1] * m,) + index
                copies.append(pltpu.make_async_copy(data[slot].at[index], dst.at[pl.ds(base, size), :], semaphore))
                base += size
        return copies

    job_copies = []
    for j, job in enumerate(jobs):
        copies = load(job['h'], h_bufs[j], job_sem.at[j])
        if cross:
            copies += load(job['src'], s_bufs[j], job_sem.at[j])
        if cfg['part_in']:
            copies += load(job['part'], p_bufs[j], job_sem.at[j])
        job_copies.append(copies)
    start_all(job_copies[0])
    qkv_copies, wo_copies, ff_groups = [], [], []
    if kind:
        if cross and own_refs:
            own = [own_refs[0].at[layer], own_refs[1].at[layer, 0], own_refs[1].at[layer, 1], own_refs[2].at[layer]]
        elif own_refs:
            own = [own_refs[0].at[layer, c] for c in range(3)] + [own_refs[1].at[layer]]
        else:
            own = []
        qkv_copies, wo_copies = attn_weight_copies(stage, own, pieces, cfg['base'], halves, w_s, wo_s, [sem.at[0], sem.at[1]])
        start_all(qkv_copies + wo_copies)
    for copies in job_copies[1:]:
        start_all(copies)
    if ff:
        ff_groups = ff_weight_copies(layer, stage, w1_ref, w2_ref, up_pieces, down_pieces, cfg['down_base'], w1_s, w2_s,
                                     [sem.at[2 + i] for i in range(4)])
        for group in ff_groups:
            start_all(group)

    gain = norm_ref[layer, cfg['gain']][None, :]
    gain_f = norm_ref[layer, cfg['ff_gain']][None, :]
    for j, job in enumerate(jobs):
        tq, tk = job['tq'], job['tk']
        tile = TILE if tq % TILE == 0 else HALF
        h_ref, o_ref, out = h_bufs[j], o_bufs[j], outs[j]
        wait_all(job_copies[j])
        if kind:
            if j == 0:
                wait_all(qkv_copies)
            if cross:
                project(h_ref, gain, w_s, slice(0, ncol), 0, tq, tile, [q_s], npair)
                project(s_bufs[j], None, w_s, slice(ncol, 3 * ncol), 0, tk, TILE, [k_s, v_s], npair)
            else:
                project(h_ref, gain, w_s, slice(0, 3 * ncol), 0, tq, tile, [q_s, k_s, v_s], npair)
                if tk > tq:
                    project(h_ref, gain, w_s, slice(ncol, 3 * ncol), tq, tk - tq, tile, [k_s, v_s], npair)
            if job['full']:
                attention(job, npair, lens[2 * m], 0, HALF, m, q_s, k_s, v_s, km_s, vx_s, ctx_s)
            else:
                attention(job, npair, lens[1], HALF * m, HALF * (1 - m), m, q_s, k_s, v_s, km_s, vx_s, ctx_s)
            if j == 0:
                wait_all(wo_copies)
        if ff and kind and j == 0:
            for group in ff_groups:
                wait_all(group)

        def finish(rows, value, o_ref=o_ref, out=out):
            if final_ref is not None:
                value = norm_rows(value, final_ref[...])
            o_ref[rows, :] = value
            pltpu.make_async_copy(o_ref.at[rows, :], out.at[rows, :], out_sem).start()

        def out_tile(i, carry, h_ref=h_ref, tile=tile, finish=finish, j=j):
            rows = rows_at(i, tile)
            h1 = h_ref[rows, :]
            if kind:
                ctx = jnp.concatenate([ctx_s[pair, rows, :] for pair in range(npair)], axis=1)
                update = dot(ctx, wo_s[...])
                if cfg['part_in']:
                    update = update + p_bufs[j][rows, :]
                if cfg['part_out']:
                    finish(rows, update)
                    return carry
                h1 = (h1.astype(jnp.float32) + update).astype(jnp.bfloat16)
            if ff:
                h1 = ff_rows(h1, gain_f, w1_s, w2_s)
            finish(rows, h1)
            return carry

        first = 0
        if ff and not kind and j == 0:
            finish(pl.ds(0, tile), ff_rows(h_ref[:tile, :], gain_f, w1_s, w2_s, ff_groups))
            first = 1
        if tq // tile > first:
            lax.fori_loop(first, tq // tile, out_tile, 0)
    for j in range(len(jobs)):
        pltpu.make_async_copy(o_bufs[j], outs[j], out_sem).wait()


FULL_CHUNKS = [(list(range(i + 1)), {i: 'diag'}) for i in range(4)]
MID_CHUNKS = [([0, 2], {0: 'diag', 2: 1}), ([0, 1, 2, 3], {1: 'diag', 3: 0})]


def run_block(lens, norms, layer, kind, jobs, data, *, gain=0, ff_gain=0, own=(), pieces=(), base=0, part_in=False, part_out=False,
              ff=None, down_base=0, final_gain=None):
    halves = ((0,) if own else ()) + ((1,) if pieces else ())
    nh, bf = len(halves), jnp.bfloat16
    npair = 3 * nh
    cfg = dict(layer=layer, kind=kind, halves=halves, ff=ff is not None, jobs=jobs, ndata=len(data), nown=len(own), npiece=len(pieces),
               base=base, down_base=down_base, gain=gain, ff_gain=ff_gain, part_in=part_in, part_out=part_out, final=final_gain is not None)
    vm = pl.BlockSpec(memory_space=pltpu.VMEM)
    hbm = pl.BlockSpec(memory_space=pl.ANY)
    head = [norms] + ([final_gain.reshape(1, D)] if final_gain is not None else [])
    rest = list(data) + list(own) + list(pieces)
    if ff is not None:
        rest += [ff[0], ff[1]] + list(ff[2]) + list(ff[3])
    odt = jnp.float32 if part_out else bf
    tq, tk = max(job['tq'] for job in jobs), max(job['tk'] for job in jobs)
    scratch = [pltpu.VMEM((job['tk'] if kind == 'self' else job['tq'], D), bf) for job in jobs]
    if kind == 'cross':
        scratch += [pltpu.VMEM((job['tk'], D), bf) for job in jobs]
    if part_in:
        scratch += [pltpu.VMEM((job['tq'], D), jnp.float32) for job in jobs]
    scratch += [pltpu.VMEM((job['tq'], D), odt) for job in jobs]
    if kind:
        scratch += [pltpu.VMEM(shape, bf) for shape in [
            (D, npair * LANES * 3), (HALF * nh, D), (npair, tq, LANES), (npair, tk, LANES), (npair, tk, LANES),
            (tk, LANES), (2 * tk, 2 * LANES), (npair, tq, LANES)]]
    if ff is not None:
        scratch += [pltpu.VMEM((D, FF), bf), pltpu.VMEM((FF, D), bf)]
    scratch += [pltpu.SemaphoreType.DMA((6,)), pltpu.SemaphoreType.DMA((2,)), pltpu.SemaphoreType.DMA]
    scores = sum(job['tq'] * job['tk'] * npair * 2 for job in jobs)
    rows_q = sum(job['tq'] for job in jobs)
    flops = scores * 512 + 8 * D * HALF * nh * rows_q + (4 * D * FF * rows_q if ff is not None else 0)
    nbytes = 4 * D * rows_q + 8 * D * HALF * nh + (4 * D * FF if ff is not None else 0)
    return pl.pallas_call(
        functools.partial(block_kernel, cfg),
        out_shape=[jax.ShapeDtypeStruct((job['tq'], D), odt) for job in jobs],
        in_specs=[pl.BlockSpec(memory_space=pltpu.SMEM)] + [vm] * len(head) + [hbm] * len(rest),
        out_specs=[hbm] * len(jobs),
        scratch_shapes=scratch,
        compiler_params=pltpu.CompilerParams(vmem_limit_bytes=VMEM_LIMIT),
        cost_estimate=pl.CostEstimate(flops=flops, bytes_accessed=nbytes, transcendentals=scores),
    )(lens, *head, *rest)


def solution(mesh):
    row_spec = P(('data', 'stage'), None, None)
    len_spec = P(('data', 'stage'))
    qkv_spec = P(None, None, None, 'model')
    col_spec = P(None, None, 'model')
    row_w_spec = P(None, 'model', None)
    rep_spec = P()
    in_specs_all = (row_spec, len_spec, row_spec, qkv_spec, row_w_spec, col_spec, row_w_spec, rep_spec, rep_spec,
                    qkv_spec, row_w_spec, col_spec, qkv_spec, row_w_spec, col_spec, row_w_spec, rep_spec)
    perms = dict(y=('model', [(0, 1), (1, 0)]), x=('stage', [(i, i ^ 2) for i in range(4)]), c=('stage', [(i, i ^ 1) for i in range(4)]))

    def permute(kind, value):
        return lax.ppermute(value, *perms[kind])

    def spread(pack):
        first = permute('y', pack)
        second = permute('x', first)
        return [first, second, permute('c', first), permute('c', second)]

    def local_step(x_enc, enc_len, y_dec, enc_wqkv, enc_wo, enc_w1, enc_w2, enc_norm, enc_final,
                   dec_wqkv, dec_wo, crs_wq, crs_wkv, crs_wo, dec_w1, dec_w2, dec_norm):
        src, tgt = x_enc.shape[1], y_dec.shape[1]
        enc_qkv_t, dec_qkv_t, crs_kv_t = [jnp.transpose(w, (0, 2, 1, 3)) for w in (enc_wqkv, dec_wqkv, crs_wkv)]
        pair_len = permute('x', enc_len)

        sources_a = [enc_qkv_t, enc_wo, enc_w1, enc_w2, dec_qkv_t, dec_wo]
        sources_b = sources_a + [crs_wq, crs_kv_t, crs_wo, dec_w1, dec_w2]

        def self_parts(slot, layer):
            return [(slot, (layer, c)) for c in range(3)] + [(slot + 1, (layer,))]

        def cross_parts(layer):
            return [(6, (layer,))] + [(7, (layer, c)) for c in range(2)] + [(8, (layer,))]

        def one(slot, layer):
            return [(slot, (layer,))]

        groups_a = [self_parts(0, 0), one(2, 0), one(3, 0), self_parts(4, 0)]
        groups_b = [self_parts(0, 1), one(2, 1), one(3, 1), cross_parts(0), one(9, 0) + one(10, 0),
                    self_parts(4, 1) + cross_parts(1), one(9, 1) + one(10, 1)]
        packs = list(run_pack(sources_a, groups_a))
        packs += list(run_pack(sources_b, groups_b))
        w = [spread(pack) for pack in packs]

        full_lead, mid_lead = (0, 2), (1, 0)
        same = [(0, 0)]

        def job(full, tq, tk, h, chunks=None, **extra):
            return dict(full=full, tq=tq, tk=tk, h=h, chunks=chunks, **extra)

        def flat(*slots_sizes):
            return [(slot, None, size, same) for slot, size in slots_sizes]

        hs, ht = src // 2, tgt // 2
        x_mid = [(0, mid_lead, hs, [(0, 1), (1, -1)])]
        x_full = [(0, full_lead, src, same)]
        y_mid = [(0, mid_lead, CHUNK, [(0, 1), (3, -1), (1, -1), (2, 1)])]
        y_full = [(0, full_lead, tgt, same)]
        e_own, d_own, c_own = (enc_qkv_t, enc_wo), (dec_qkv_t, dec_wo), (crs_wq, crs_kv_t, crs_wo)

        pd_mid, pd_full = run_block(enc_len, dec_norm, 0, 'self', [job(False, ht, tgt, y_mid, MID_CHUNKS), job(True, tgt, tgt, y_full, FULL_CHUNKS)],
                                [y_dec], own=d_own, part_out=True)
        pe_mid, pe_full = run_block(enc_len, enc_norm, 0, 'self', [job(False, hs, src, x_mid), job(True, src, src, x_full)],
                                [x_enc], own=e_own, part_out=True)
        h_mid, h_full = run_block(enc_len, enc_norm, 0, 'self',
                              [job(False, hs, src, x_mid, part=flat((1, hs))), job(True, src, src, x_full, part=flat((2, src)))],
                              [x_enc, pe_mid, pe_full], pieces=w[0], part_in=True)
        h_mid, h_full = run_block(enc_len, enc_norm, 0, '', [job(False, hs, hs, flat((0, hs))), job(True, src, src, flat((1, src)))],
                              [h_mid, h_full], ff_gain=1, ff=(enc_w1, enc_w2, w[1], w[2]))
        h_other = permute('y', h_mid)
        z_mid, = run_block(enc_len, dec_norm, 0, 'self', [job(False, ht, tgt, y_mid, MID_CHUNKS, part=flat((1, ht)))],
                       [y_dec, pd_mid], pieces=w[3], part_in=True)
        h_full, = run_block(enc_len, enc_norm, 1, 'self', [job(True, src, src, flat((0, src)))], [h_full], own=e_own, pieces=w[4])
        h_mid, = run_block(enc_len, enc_norm, 1, 'self', [job(False, hs, src, flat((0, hs), (1, hs)))], [h_mid, h_other], own=e_own, pieces=w[4])
        e1_ff = dict(ff_gain=1, ff=(enc_w1, enc_w2, w[5], w[6]), final_gain=enc_final)
        s_mid, = run_block(enc_len, enc_norm, 1, '', [job(False, hs, hs, flat((0, hs)))], [h_mid], **e1_ff)
        s_mid = permute('x', s_mid)
        s_full, = run_block(enc_len, enc_norm, 1, '', [job(True, src, src, flat((0, src)))], [h_full], **e1_ff)
        s_full = permute('x', s_full)
        s_other = permute('y', s_mid)
        z_full, = run_block(enc_len, dec_norm, 0, 'self', [job(True, tgt, tgt, y_full, FULL_CHUNKS, part=flat((1, tgt)))],
                        [y_dec, pd_full], pieces=w[3], part_in=True)

        def cross_mid(z, layer, **kwargs):
            return run_block(pair_len, dec_norm, layer, 'cross', [job(False, ht, src, flat((0, ht)), src=flat((1, hs), (2, hs)))],
                         [z, s_mid, s_other], own=c_own, gain=1, ff_gain=2, **kwargs)[0]

        def cross_full(z, layer, **kwargs):
            return run_block(pair_len, dec_norm, layer, 'cross', [job(True, tgt, src, flat((0, tgt)), src=flat((1, src)))],
                         [z, s_full], own=c_own, gain=1, ff_gain=2, **kwargs)[0]

        cross0 = dict(pieces=w[7], ff=(dec_w1, dec_w2, w[8], w[8]), down_base=D)
        cross1 = dict(pieces=w[9], base=D, ff=(dec_w1, dec_w2, w[10], w[10]), down_base=D)
        z_mid = cross_mid(z_mid, 0, **cross0)
        z_other = permute('y', z_mid)
        z_full = cross_full(z_full, 0, **cross0)
        z_full, = run_block(enc_len, dec_norm, 1, 'self', [job(True, tgt, tgt, flat((0, tgt)), FULL_CHUNKS)], [z_full], own=d_own, pieces=w[9])
        z_full = cross_full(z_full, 1, **cross1)
        z_full_other = permute('y', z_full)
        z_mid, = run_block(enc_len, dec_norm, 1, 'self', [job(False, ht, tgt, flat((0, ht), (1, ht)), MID_CHUNKS)], [z_mid, z_other],
                       own=d_own, pieces=w[9])
        z_mid = cross_mid(z_mid, 1, **cross1)
        z_mid_other = permute('y', z_mid)

        first = lax.axis_index('model') == 0
        a, b, oa, ob = z_mid[:CHUNK], z_mid[CHUNK:], z_mid_other[:CHUNK], z_mid_other[CHUNK:]
        row_mid = jnp.where(first, jnp.concatenate([a, oa, ob, b], axis=0), jnp.concatenate([oa, a, b, ob], axis=0))
        return jnp.stack([jnp.where(first, z_full, z_full_other), row_mid, jnp.where(first, z_full_other, z_full)])

    return jax.shard_map(local_step, mesh=mesh, in_specs=in_specs_all, out_specs=row_spec, check_vma=False)
```

```python
import functools
import math

import jax
import jax.numpy as jnp
from jax import lax
from jax.experimental import pallas as pl
from jax.experimental.pallas import tpu as pltpu
from jax.sharding import PartitionSpec as P


D = 768
HALF = 384
FF = 3072
NORM_EPS = 1e-6
NEG_BIG = -1e30
EXP_SCALE = 0.125 * math.log2(math.e)
GELU_C = math.sqrt(2.0 / math.pi)
PIECE_XOR = (0, 2, 1, 3)
QROWS = 192
OROWS = 96
TILE = 256
CHUNK = 256
LANES = 128
SUB = 16
HEAD_DIM = 64
VMEM_LIMIT = 60 * 1024 * 1024


def norm_rows(h, gain):
    hf = h.astype(jnp.float32)
    inv = lax.rsqrt(jnp.mean(hf * hf, axis=-1, keepdims=True) + NORM_EPS)
    return (hf * inv * gain).astype(jnp.bfloat16)


def gelu(x):
    return x * (0.5 + 0.5 * jnp.tanh(GELU_C * (x + 0.044715 * (x * x * x))))


def dot(a, b):
    return jnp.dot(a, b, preferred_element_type=jnp.float32)


def dot_t(a, b):
    return lax.dot_general(a, b, (((1,), (1,)), ((), ())), preferred_element_type=jnp.float32)


def runs_of(chunks):
    runs = []
    for c in chunks:
        if runs and runs[-1][0] + runs[-1][1] == c:
            runs[-1] = (runs[-1][0], runs[-1][1] + 1)
        else:
            runs.append((c, 1))
    return runs


def row_copies(src, dst, sem, step):
    rows = src.shape[0]
    return [pltpu.make_async_copy(src.at[pl.ds(r, step), :], dst.at[pl.ds(r, step), :], sem) for r in range(0, rows, step)]


def attn_weight_copies(stage, own, pieces, base, halves, w_s, wo_s, sems):
    ncol = HALF * len(halves)
    off = ncol - HALF
    qkv, out = [], []
    if own:
        for c, src in enumerate(own[:-1]):
            qkv += row_copies(src, w_s.at[:, pl.ds(c * ncol, HALF)], sems[0], QROWS)
        out += row_copies(own[-1], wo_s.at[pl.ds(0, HALF), :], sems[1], OROWS)
    for piece, mask in zip(pieces, PIECE_XOR):
        quarter = stage ^ mask
        r0 = pl.multiple_of(quarter * QROWS, QROWS)
        for c in range(3):
            qkv.append(pltpu.make_async_copy(piece.at[pl.ds(base + c * QROWS, QROWS), :],
                                             w_s.at[pl.ds(r0, QROWS), pl.ds(c * ncol + off, HALF)], sems[0]))
        r1 = pl.multiple_of(off + quarter * OROWS, OROWS)
        for c in range(2):
            out.append(pltpu.make_async_copy(piece.at[pl.ds(base + 3 * QROWS + c * OROWS, OROWS), :],
                                             wo_s.at[pl.ds(r1, OROWS), pl.ds(c * HALF, HALF)], sems[1]))
    return qkv, out


def ff_weight_copies(layer, stage, w1_ref, w2_ref, up_pieces, down_pieces, down_base, w1_s, w2_s, sems):
    hf = FF // 2
    own_up = row_copies(w1_ref.at[layer], w1_s.at[:, pl.ds(0, hf)], sems[0], OROWS // 2)
    own_down = row_copies(w2_ref.at[layer], w2_s.at[pl.ds(0, hf), :], sems[1], OROWS)
    up, down = [], []
    for i, mask in enumerate(PIECE_XOR):
        quarter = stage ^ mask
        r0 = pl.multiple_of(quarter * QROWS, QROWS)
        for c in range(4):
            up.append(pltpu.make_async_copy(up_pieces[i].at[pl.ds(c * QROWS, QROWS), :],
                                            w1_s.at[pl.ds(r0, QROWS), pl.ds(hf + c * HALF, HALF)], sems[2]))
        r1 = pl.multiple_of(hf + quarter * HALF, HALF)
        for c in range(2):
            down.append(pltpu.make_async_copy(down_pieces[i].at[pl.ds(down_base + c * HALF, HALF), :],
                                              w2_s.at[pl.ds(r1, HALF), pl.ds(c * HALF, HALF)], sems[3]))
    return [own_up, own_down, up, down]


def start_all(copies):
    for copy in copies:
        copy.start()


def wait_all(copies):
    for copy in copies:
        copy.wait()


def ff_rows(h1, gain, w1_s, w2_s, waits=None):
    xn = norm_rows(h1, gain)
    acc = None
    for c in range(FF // D):
        cols = slice(c * D, (c + 1) * D)
        second = c * D >= FF // 2
        if waits is not None and c in (0, FF // D // 2):
            wait_all(waits[2 * second])
        act = gelu(dot(xn, w1_s[:, cols])).astype(jnp.bfloat16)
        if waits is not None and c in (0, FF // D // 2):
            wait_all(waits[2 * second + 1])
        term = dot(act, w2_s[cols, :])
        acc = term if acc is None else acc + term
    return (h1.astype(jnp.float32) + acc).astype(jnp.bfloat16)


def pack_kernel(cfg, *refs):
    ins, outs, sem = refs[:cfg['nin']], refs[cfg['nin']:-1], refs[-1]
    stage = lax.axis_index('stage')
    copies = []
    for out, parts in zip(outs, cfg['groups']):
        base = 0
        for slot, index in parts:
            ref = ins[slot]
            size = ref.shape[-2] // 4
            for c in range(ref.shape[-1] // HALF):
                src = ref.at[index + (pl.ds(pl.multiple_of(stage * size, size), size), pl.ds(c * HALF, HALF))]
                copies.append(pltpu.make_async_copy(src, out.at[pl.ds(base, size), :], sem))
                base += size
    start_all(copies)
    wait_all(copies)


def group_rows(sources, parts):
    return sum(sources[slot].shape[-2] * sources[slot].shape[-1] // (4 * HALF) for slot, _ in parts)


def run_pack(sources, groups):
    hbm = pl.BlockSpec(memory_space=pl.ANY)
    vm = pl.BlockSpec(memory_space=pltpu.VMEM)
    shapes = [jax.ShapeDtypeStruct((group_rows(sources, parts), HALF), jnp.bfloat16) for parts in groups]
    return pl.pallas_call(
        functools.partial(pack_kernel, dict(nin=len(sources), groups=groups)),
        out_shape=shapes,
        in_specs=[hbm] * len(sources),
        out_specs=[vm] * len(groups),
        scratch_shapes=[pltpu.SemaphoreType.DMA],
        compiler_params=pltpu.CompilerParams(vmem_limit_bytes=VMEM_LIMIT),
        cost_estimate=pl.CostEstimate(flops=0, bytes_accessed=sum(4 * shape.size for shape in shapes), transcendentals=0),
    )(*sources)


def rows_at(i, size):
    return pl.ds(pl.multiple_of(i * size, size), size)


def project(h_ref, gain, w_s, cols, first, count, tile, dests, npair):
    def body(i, carry):
        rows = rows_at(first // tile + i, tile)
        x = h_ref[rows, :] if gain is None else norm_rows(h_ref[rows, :], gain)
        value = dot(x, w_s[:, cols])
        for d, dst in enumerate(dests):
            for pair in range(npair):
                col = (d * npair + pair) * LANES
                dst[pair, rows, :] = value[:, col:col + LANES].astype(jnp.bfloat16)
        return carry

    lax.fori_loop(0, count // tile, body, 0)


def attention(job, pairs, src_len, off_a, off_b, model_idx, q_s, k_s, v_s, km_s, vx_s, ctx_s):
    tq, tk, chunk_plan = job['tq'], job['tk'], job['chunks']
    causal = chunk_plan is not None
    qb = LANES
    npair = pairs
    lane = lax.broadcasted_iota(jnp.int32, (1, LANES), 1)
    lo_f = jnp.where(lane < HEAD_DIM, 1.0, 0.0).astype(jnp.float32)
    masks_f = (lo_f, 1.0 - lo_f)
    masks_b = [mask.astype(jnp.bfloat16) for mask in masks_f]
    nchunk = tk // CHUNK

    def pair_body(pair, carry):
        if not causal:
            k_first = jnp.where(off_a == 0, k_s[pair, 0:SUB, :].astype(jnp.float32)[0:1],
                                k_s[pair, HALF:HALF + SUB, :].astype(jnp.float32)[0:1])
        for c in range(nchunk):
            rows = slice(c * CHUNK, (c + 1) * CHUNK)
            v_f = v_s[pair, rows, :].astype(jnp.float32)
            ones = jnp.ones((CHUNK, LANES), jnp.float32)
            if not causal:
                idx = lax.broadcasted_iota(jnp.int32, (CHUNK, LANES), 0) + c * CHUNK
                pos = jnp.where(idx < HALF, idx + off_a, idx + (off_b - HALF))
                ok = pos < src_len
                km_s[rows, :] = jnp.where(ok, k_s[pair, rows, :].astype(jnp.float32), k_first).astype(jnp.bfloat16)
                v_f = jnp.where(ok, v_f, 0.0)
                ones = jnp.where(ok, ones, 0.0)
            for head, mask in enumerate(masks_f):
                vrows = slice((2 * c + head) * CHUNK, (2 * c + head + 1) * CHUNK)
                vx_s[vrows, :LANES] = (v_f * mask).astype(jnp.bfloat16)
                vx_s[vrows, LANES:] = (ones * mask).astype(jnp.bfloat16)
        for b in range(tq // qb):
            rows = slice(b * qb, (b + 1) * qb)
            qp = q_s[pair, rows, :]
            q2 = jnp.concatenate([qp * mask for mask in masks_b], axis=0)
            chunks, masks = chunk_plan[b * qb // CHUNK] if causal else (list(range(nchunk)), {})
            parts = []
            for start, count in runs_of(chunks):
                krows = slice(start * CHUNK, (start + count) * CHUNK)
                s_run = dot_t(q2, k_s[pair, krows, :] if causal else km_s[krows, :])
                for j in range(count):
                    s_c = s_run[:, j * CHUNK:(j + 1) * CHUNK]
                    kind = masks.get(start + j)
                    if kind == 'diag':
                        q_idx = lax.broadcasted_iota(jnp.int32, (2 * qb, CHUNK), 0)
                        q_idx = jnp.where(q_idx < qb, q_idx, q_idx - qb) + (b * qb % CHUNK)
                        k_idx = lax.broadcasted_iota(jnp.int32, (2 * qb, CHUNK), 1)
                        s_c = jnp.where(k_idx <= q_idx, s_c, NEG_BIG)
                    elif kind is not None:
                        s_c = jnp.where(model_idx == kind, s_c, NEG_BIG)
                    parts.append(s_c)
            top = functools.reduce(jnp.maximum, parts)
            top = jnp.max(top, axis=-1, keepdims=True)
            probs = [jnp.exp2((part - top) * EXP_SCALE).astype(jnp.bfloat16) for part in parts]
            terms = []
            for start, count in runs_of(chunks):
                used, probs = probs[:count], probs[count:]
                lhs = [half for prob in used for half in (prob[:qb], prob[qb:])]
                terms.append(dot(jnp.concatenate(lhs, axis=1), vx_s[2 * start * CHUNK:2 * (start + count) * CHUNK, :]))
            total = functools.reduce(jnp.add, terms)
            ctx_s[pair, rows, :] = (total[:, :LANES] / total[:, LANES:]).astype(jnp.bfloat16)
        return carry

    lax.fori_loop(0, npair, pair_body, 0)


def block_kernel(cfg, *refs):
    it = iter(refs)

    def take(n):
        return [next(it) for _ in range(n)]

    layer, kind, halves, ff, jobs = cfg['layer'], cfg['kind'], cfg['halves'], cfg['ff'], cfg['jobs']
    cross = kind == 'cross'
    nh = len(halves)
    npair, ncol = 3 * nh, HALF * nh
    lens, norm_in = take(2)
    final_in = take(1)[0] if cfg['final'] else None
    data = take(cfg['ndata'])
    own_refs = take(cfg['nown'])
    pieces = take(cfg['npiece'])
    if ff:
        w1_ref, w2_ref = take(2)
        up_pieces, down_pieces = take(4), take(4)
    outs = take(len(jobs))
    h_bufs = take(len(jobs))
    s_bufs = take(len(jobs)) if cross else None
    p_bufs = take(len(jobs)) if cfg['part_in'] else None
    o_bufs = take(len(jobs))
    if kind:
        w_s, wo_s, q_s, k_s, v_s, km_s, vx_s, ctx_s = take(8)
    if ff:
        w1_s, w2_s = take(2)
    norm_ref = take(1)[0]
    final_ref = take(1)[0] if cfg['final'] else None
    sem, job_sem, out_sem = take(3)
    m, stage = lax.axis_index('model'), lax.axis_index('stage')

    def load(parts, dst, semaphore):
        copies, base = [], 0
        for slot, lead, size, steps in parts:
            for a, b in steps:
                start = pl.multiple_of((a + b * m) * size, size) if lead is not None else 0
                src = data[slot]
                if lead is not None:
                    src = src.at[lead[0] + lead[1] * m]
                copies += row_copies(src.at[pl.ds(start, size), :], dst.at[pl.ds(base, size), :], semaphore, LANES)
                base += size
        return copies

    job_copies = []
    for j, job in enumerate(jobs):
        copies = load(job['h'], h_bufs[j], job_sem.at[j])
        if cross:
            copies += load(job['src'], s_bufs[j], job_sem.at[j])
        if cfg['part_in']:
            copies += load(job['part'], p_bufs[j], job_sem.at[j])
        job_copies.append(copies)
    job_copies[0].append(pltpu.make_async_copy(norm_in, norm_ref, job_sem.at[0]))
    if final_ref is not None:
        job_copies[0].append(pltpu.make_async_copy(final_in, final_ref, job_sem.at[0]))
    start_all(job_copies[0])
    qkv_copies, wo_copies, ff_groups = [], [], []
    if kind:
        if cross and own_refs:
            own = [own_refs[0].at[layer], own_refs[1].at[layer, 0], own_refs[1].at[layer, 1], own_refs[2].at[layer]]
        elif own_refs:
            own = [own_refs[0].at[layer, c] for c in range(3)] + [own_refs[1].at[layer]]
        else:
            own = []
        qkv_copies, wo_copies = attn_weight_copies(stage, own, pieces, cfg['base'], halves, w_s, wo_s, [sem.at[0], sem.at[1]])
        start_all(qkv_copies + wo_copies)
    for copies in job_copies[1:]:
        start_all(copies)
    if ff:
        ff_groups = ff_weight_copies(layer, stage, w1_ref, w2_ref, up_pieces, down_pieces, cfg['down_base'], w1_s, w2_s,
                                     [sem.at[2 + i] for i in range(4)])
        for group in ff_groups:
            start_all(group)

    wait_all(job_copies[0])
    gain = norm_ref[layer, cfg['gain']][None, :]
    gain_f = norm_ref[layer, cfg['ff_gain']][None, :]
    for j, job in enumerate(jobs):
        tq, tk = job['tq'], job['tk']
        tile = TILE if tq % TILE == 0 else HALF
        h_ref, o_ref, out = h_bufs[j], o_bufs[j], outs[j]
        if j > 0:
            wait_all(job_copies[j])
        if kind:
            if j == 0:
                wait_all(qkv_copies)
            if cross:
                project(h_ref, gain, w_s, slice(0, ncol), 0, tq, tile, [q_s], npair)
                project(s_bufs[j], None, w_s, slice(ncol, 3 * ncol), 0, tk, TILE, [k_s, v_s], npair)
            else:
                project(h_ref, gain, w_s, slice(0, 3 * ncol), 0, tq, tile, [q_s, k_s, v_s], npair)
                if tk > tq:
                    project(h_ref, gain, w_s, slice(ncol, 3 * ncol), tq, tk - tq, tile, [k_s, v_s], npair)
            if job['full']:
                attention(job, npair, lens[2 * m], 0, HALF, m, q_s, k_s, v_s, km_s, vx_s, ctx_s)
            else:
                attention(job, npair, lens[1], HALF * m, HALF * (1 - m), m, q_s, k_s, v_s, km_s, vx_s, ctx_s)
            if j == 0:
                wait_all(wo_copies)
        if ff and kind and j == 0:
            for group in ff_groups:
                wait_all(group)

        def finish(rows, value, o_ref=o_ref, out=out):
            if final_ref is not None:
                value = norm_rows(value, final_ref[...][None, :])
            o_ref[rows, :] = value
            pltpu.make_async_copy(o_ref.at[rows, :], out.at[rows, :], out_sem).start()

        def out_tile(i, carry, h_ref=h_ref, tile=tile, finish=finish, j=j):
            rows = rows_at(i, tile)
            h1 = h_ref[rows, :]
            if kind:
                ctx = jnp.concatenate([ctx_s[pair, rows, :] for pair in range(npair)], axis=1)
                update = dot(ctx, wo_s[...])
                if cfg['part_in']:
                    update = update + p_bufs[j][rows, :]
                if cfg['part_out']:
                    finish(rows, update)
                    return carry
                h1 = (h1.astype(jnp.float32) + update).astype(jnp.bfloat16)
            if ff:
                h1 = ff_rows(h1, gain_f, w1_s, w2_s)
            finish(rows, h1)
            return carry

        first = 0
        if ff and not kind and j == 0:
            finish(pl.ds(0, tile), ff_rows(h_ref[:tile, :], gain_f, w1_s, w2_s, ff_groups))
            first = 1
        if tq // tile > first:
            lax.fori_loop(first, tq // tile, out_tile, 0)
    for j in range(len(jobs)):
        pltpu.make_async_copy(o_bufs[j], outs[j], out_sem).wait()


FULL_CHUNKS = [(list(range(i + 1)), {i: 'diag'}) for i in range(4)]
MID_CHUNKS = [([0, 2], {0: 'diag', 2: 1}), ([0, 1, 2, 3], {1: 'diag', 3: 0})]


def run_block(lens, norms, layer, kind, jobs, data, *, gain=0, ff_gain=0, own=(), pieces=(), base=0, part_in=False, part_out=False,
              ff=None, down_base=0, final_gain=None):
    halves = ((0,) if own else ()) + ((1,) if pieces else ())
    nh, bf = len(halves), jnp.bfloat16
    npair = 3 * nh
    cfg = dict(layer=layer, kind=kind, halves=halves, ff=ff is not None, jobs=jobs, ndata=len(data), nown=len(own), npiece=len(pieces),
               base=base, down_base=down_base, gain=gain, ff_gain=ff_gain, part_in=part_in, part_out=part_out, final=final_gain is not None)
    hbm = pl.BlockSpec(memory_space=pl.ANY)
    head = [norms] + ([final_gain] if final_gain is not None else [])
    rest = head + list(data) + list(own) + list(pieces)
    if ff is not None:
        rest += [ff[0], ff[1]] + list(ff[2]) + list(ff[3])
    odt = jnp.float32 if part_out else bf
    tq, tk = max(job['tq'] for job in jobs), max(job['tk'] for job in jobs)
    scratch = [pltpu.VMEM((job['tk'] if kind == 'self' else job['tq'], D), bf) for job in jobs]
    if kind == 'cross':
        scratch += [pltpu.VMEM((job['tk'], D), bf) for job in jobs]
    if part_in:
        scratch += [pltpu.VMEM((job['tq'], D), jnp.float32) for job in jobs]
    scratch += [pltpu.VMEM((job['tq'], D), odt) for job in jobs]
    if kind:
        scratch += [pltpu.VMEM(shape, bf) for shape in [
            (D, npair * LANES * 3), (HALF * nh, D), (npair, tq, LANES), (npair, tk, LANES), (npair, tk, LANES),
            (tk, LANES), (2 * tk, 2 * LANES), (npair, tq, LANES)]]
    if ff is not None:
        scratch += [pltpu.VMEM((D, FF), bf), pltpu.VMEM((FF, D), bf)]
    scratch += [pltpu.VMEM(value.shape, jnp.float32) for value in head]
    scratch += [pltpu.SemaphoreType.DMA((6,)), pltpu.SemaphoreType.DMA((2,)), pltpu.SemaphoreType.DMA]
    scores = sum(job['tq'] * job['tk'] * npair * 2 for job in jobs)
    rows_q = sum(job['tq'] for job in jobs)
    flops = scores * 512 + 8 * D * HALF * nh * rows_q + (4 * D * FF * rows_q if ff is not None else 0)
    nbytes = 4 * D * rows_q + 8 * D * HALF * nh + (4 * D * FF if ff is not None else 0)
    return pl.pallas_call(
        functools.partial(block_kernel, cfg),
        out_shape=[jax.ShapeDtypeStruct((job['tq'], D), odt) for job in jobs],
        in_specs=[pl.BlockSpec(memory_space=pltpu.SMEM)] + [hbm] * len(rest),
        out_specs=[hbm] * len(jobs),
        scratch_shapes=scratch,
        compiler_params=pltpu.CompilerParams(vmem_limit_bytes=VMEM_LIMIT),
        cost_estimate=pl.CostEstimate(flops=flops, bytes_accessed=nbytes, transcendentals=scores),
    )(lens, *rest)


def solution(mesh):
    row_spec = P(('data', 'stage'), None, None)
    len_spec = P(('data', 'stage'))
    qkv_spec = P(None, None, None, 'model')
    col_spec = P(None, None, 'model')
    row_w_spec = P(None, 'model', None)
    rep_spec = P()
    in_specs_all = (row_spec, len_spec, row_spec, qkv_spec, row_w_spec, col_spec, row_w_spec, rep_spec, rep_spec,
                    qkv_spec, row_w_spec, col_spec, qkv_spec, row_w_spec, col_spec, row_w_spec, rep_spec)
    perms = dict(y=('model', [(0, 1), (1, 0)]), x=('stage', [(i, i ^ 2) for i in range(4)]), c=('stage', [(i, i ^ 1) for i in range(4)]))

    def permute(kind, value):
        return lax.ppermute(value, *perms[kind])

    def spread(pack):
        first = permute('y', pack)
        second = permute('x', first)
        return [first, second, permute('c', first), permute('c', second)]

    def local_step(x_enc, enc_len, y_dec, enc_wqkv, enc_wo, enc_w1, enc_w2, enc_norm, enc_final,
                   dec_wqkv, dec_wo, crs_wq, crs_wkv, crs_wo, dec_w1, dec_w2, dec_norm):
        src, tgt = x_enc.shape[1], y_dec.shape[1]
        enc_qkv_t, dec_qkv_t, crs_kv_t = [jnp.transpose(w, (0, 2, 1, 3)) for w in (enc_wqkv, dec_wqkv, crs_wkv)]
        pair_len = permute('x', enc_len)

        sources_a = [enc_qkv_t, enc_wo, enc_w1, enc_w2, dec_qkv_t, dec_wo]
        sources_b = sources_a + [crs_wq, crs_kv_t, crs_wo, dec_w1, dec_w2]

        def self_parts(slot, layer):
            return [(slot, (layer, c)) for c in range(3)] + [(slot + 1, (layer,))]

        def cross_parts(layer):
            return [(6, (layer,))] + [(7, (layer, c)) for c in range(2)] + [(8, (layer,))]

        def one(slot, layer):
            return [(slot, (layer,))]

        groups_a = [self_parts(0, 0), one(2, 0), one(3, 0), self_parts(4, 0)]
        groups_b = [self_parts(0, 1), one(2, 1), one(3, 1), cross_parts(0), one(9, 0) + one(10, 0),
                    self_parts(4, 1) + cross_parts(1), one(9, 1) + one(10, 1)]
        packs = list(run_pack(sources_a, groups_a))
        packs += list(run_pack(sources_b, groups_b))
        w = [spread(pack) for pack in packs]

        full_lead, mid_lead = (0, 2), (1, 0)
        same = [(0, 0)]

        def job(full, tq, tk, h, chunks=None, **extra):
            return dict(full=full, tq=tq, tk=tk, h=h, chunks=chunks, **extra)

        def flat(*slots_sizes):
            return [(slot, None, size, same) for slot, size in slots_sizes]

        hs, ht = src // 2, tgt // 2
        x_mid = [(0, mid_lead, hs, [(0, 1), (1, -1)])]
        x_full = [(0, full_lead, src, same)]
        y_mid = [(0, mid_lead, CHUNK, [(0, 1), (3, -1), (1, -1), (2, 1)])]
        y_full = [(0, full_lead, tgt, same)]
        e_own, d_own, c_own = (enc_qkv_t, enc_wo), (dec_qkv_t, dec_wo), (crs_wq, crs_kv_t, crs_wo)

        pd_mid, pd_full = run_block(enc_len, dec_norm, 0, 'self', [job(False, ht, tgt, y_mid, MID_CHUNKS), job(True, tgt, tgt, y_full, FULL_CHUNKS)],
                                [y_dec], own=d_own, part_out=True)
        pe_mid, pe_full = run_block(enc_len, enc_norm, 0, 'self', [job(False, hs, src, x_mid), job(True, src, src, x_full)],
                                [x_enc], own=e_own, part_out=True)
        h_mid, h_full = run_block(enc_len, enc_norm, 0, 'self',
                              [job(False, hs, src, x_mid, part=flat((1, hs))), job(True, src, src, x_full, part=flat((2, src)))],
                              [x_enc, pe_mid, pe_full], pieces=w[0], part_in=True)
        h_mid, h_full = run_block(enc_len, enc_norm, 0, '', [job(False, hs, hs, flat((0, hs))), job(True, src, src, flat((1, src)))],
                              [h_mid, h_full], ff_gain=1, ff=(enc_w1, enc_w2, w[1], w[2]))
        h_other = permute('y', h_mid)
        z_mid, = run_block(enc_len, dec_norm, 0, 'self', [job(False, ht, tgt, y_mid, MID_CHUNKS, part=flat((1, ht)))],
                       [y_dec, pd_mid], pieces=w[3], part_in=True)
        h_full, = run_block(enc_len, enc_norm, 1, 'self', [job(True, src, src, flat((0, src)))], [h_full], own=e_own, pieces=w[4])
        h_mid, = run_block(enc_len, enc_norm, 1, 'self', [job(False, hs, src, flat((0, hs), (1, hs)))], [h_mid, h_other], own=e_own, pieces=w[4])
        e1_ff = dict(ff_gain=1, ff=(enc_w1, enc_w2, w[5], w[6]), final_gain=enc_final)
        s_mid, = run_block(enc_len, enc_norm, 1, '', [job(False, hs, hs, flat((0, hs)))], [h_mid], **e1_ff)
        s_mid = permute('x', s_mid)
        s_full, = run_block(enc_len, enc_norm, 1, '', [job(True, src, src, flat((0, src)))], [h_full], **e1_ff)
        s_full = permute('x', s_full)
        s_other = permute('y', s_mid)
        z_full, = run_block(enc_len, dec_norm, 0, 'self', [job(True, tgt, tgt, y_full, FULL_CHUNKS, part=flat((1, tgt)))],
                        [y_dec, pd_full], pieces=w[3], part_in=True)

        def cross_mid(z, layer, **kwargs):
            return run_block(pair_len, dec_norm, layer, 'cross', [job(False, ht, src, flat((0, ht)), src=flat((1, hs), (2, hs)))],
                         [z, s_mid, s_other], own=c_own, gain=1, ff_gain=2, **kwargs)[0]

        def cross_full(z, layer, **kwargs):
            return run_block(pair_len, dec_norm, layer, 'cross', [job(True, tgt, src, flat((0, tgt)), src=flat((1, src)))],
                         [z, s_full], own=c_own, gain=1, ff_gain=2, **kwargs)[0]

        cross0 = dict(pieces=w[7], ff=(dec_w1, dec_w2, w[8], w[8]), down_base=D)
        cross1 = dict(pieces=w[9], base=D, ff=(dec_w1, dec_w2, w[10], w[10]), down_base=D)
        z_mid = cross_mid(z_mid, 0, **cross0)
        z_other = permute('y', z_mid)
        z_full = cross_full(z_full, 0, **cross0)
        z_full, = run_block(enc_len, dec_norm, 1, 'self', [job(True, tgt, tgt, flat((0, tgt)), FULL_CHUNKS)], [z_full], own=d_own, pieces=w[9])
        z_full = cross_full(z_full, 1, **cross1)
        z_full_other = permute('y', z_full)
        z_mid, = run_block(enc_len, dec_norm, 1, 'self', [job(False, ht, tgt, flat((0, ht), (1, ht)), MID_CHUNKS)], [z_mid, z_other],
                       own=d_own, pieces=w[9])
        z_mid = cross_mid(z_mid, 1, **cross1)
        z_mid_other = permute('y', z_mid)

        first = lax.axis_index('model') == 0
        a, b, oa, ob = z_mid[:CHUNK], z_mid[CHUNK:], z_mid_other[:CHUNK], z_mid_other[CHUNK:]
        row_mid = jnp.where(first, jnp.concatenate([a, oa, ob, b], axis=0), jnp.concatenate([oa, a, b, ob], axis=0))
        return jnp.stack([jnp.where(first, z_full, z_full_other), row_mid, jnp.where(first, z_full_other, z_full)])

    return jax.shard_map(local_step, mesh=mesh, in_specs=in_specs_all, out_specs=row_spec, check_vma=False)
```

```python
import functools
import math

import jax
import jax.numpy as jnp
from jax import lax
from jax.experimental import pallas as pl
from jax.experimental.pallas import tpu as pltpu
from jax.sharding import PartitionSpec as P


D = 768
HALF = 384
FF = 3072
NORM_EPS = 1e-6
NEG_BIG = -1e30
EXP_SCALE = 0.125 * math.log2(math.e)
GELU_C = math.sqrt(2.0 / math.pi)
PIECE_XOR = (0, 2, 1, 3)
QROWS = 192
OROWS = 96
TILE = 256
CHUNK = 256
LANES = 128
SUB = 16
HEAD_DIM = 64
VMEM_LIMIT = 60 * 1024 * 1024


def norm_rows(h, gain):
    hf = h.astype(jnp.float32)
    inv = lax.rsqrt(jnp.mean(hf * hf, axis=-1, keepdims=True) + NORM_EPS)
    return (hf * inv * gain).astype(jnp.bfloat16)


def gelu(x):
    return x * (0.5 + 0.5 * jnp.tanh(GELU_C * (x + 0.044715 * (x * x * x))))


def dot(a, b):
    return jnp.dot(a, b, preferred_element_type=jnp.float32)


def dot_t(a, b):
    return lax.dot_general(a, b, (((1,), (1,)), ((), ())), preferred_element_type=jnp.float32)


def runs_of(chunks):
    runs = []
    for c in chunks:
        if runs and runs[-1][0] + runs[-1][1] == c:
            runs[-1] = (runs[-1][0], runs[-1][1] + 1)
        else:
            runs.append((c, 1))
    return runs


def row_copies(src, dst, sem, step):
    rows = src.shape[0]
    return [pltpu.make_async_copy(src.at[pl.ds(r, step), :], dst.at[pl.ds(r, step), :], sem) for r in range(0, rows, step)]


def attn_weight_copies(stage, own, pieces, base, halves, w_s, wo_s, sems):
    ncol = HALF * len(halves)
    off = ncol - HALF
    qkv, out = [], []
    if own:
        for c, src in enumerate(own[:-1]):
            qkv += row_copies(src, w_s.at[:, pl.ds(c * ncol, HALF)], sems[0], QROWS)
        out += row_copies(own[-1], wo_s.at[pl.ds(0, HALF), :], sems[1], OROWS)
    for piece, mask in zip(pieces, PIECE_XOR):
        quarter = stage ^ mask
        r0 = pl.multiple_of(quarter * QROWS, QROWS)
        for c in range(3):
            qkv.append(pltpu.make_async_copy(piece.at[pl.ds(base + c * QROWS, QROWS), :],
                                             w_s.at[pl.ds(r0, QROWS), pl.ds(c * ncol + off, HALF)], sems[0]))
        r1 = pl.multiple_of(off + quarter * OROWS, OROWS)
        for c in range(2):
            out.append(pltpu.make_async_copy(piece.at[pl.ds(base + 3 * QROWS + c * OROWS, OROWS), :],
                                             wo_s.at[pl.ds(r1, OROWS), pl.ds(c * HALF, HALF)], sems[1]))
    return qkv, out


def ff_weight_copies(layer, stage, w1_ref, w2_ref, up_pieces, down_pieces, down_base, w1_s, w2_s, sems):
    hf = FF // 2
    own_up = row_copies(w1_ref.at[layer], w1_s.at[:, pl.ds(0, hf)], sems[0], OROWS // 2)
    own_down = row_copies(w2_ref.at[layer], w2_s.at[pl.ds(0, hf), :], sems[1], OROWS)
    up, down = [], []
    for i, mask in enumerate(PIECE_XOR):
        quarter = stage ^ mask
        r0 = pl.multiple_of(quarter * QROWS, QROWS)
        for c in range(4):
            up.append(pltpu.make_async_copy(up_pieces[i].at[pl.ds(c * QROWS, QROWS), :],
                                            w1_s.at[pl.ds(r0, QROWS), pl.ds(hf + c * HALF, HALF)], sems[2]))
        r1 = pl.multiple_of(hf + quarter * HALF, HALF)
        for c in range(2):
            down.append(pltpu.make_async_copy(down_pieces[i].at[pl.ds(down_base + c * HALF, HALF), :],
                                              w2_s.at[pl.ds(r1, HALF), pl.ds(c * HALF, HALF)], sems[3]))
    return [own_up, own_down, up, down]


def start_all(copies):
    for copy in copies:
        copy.start()


def wait_all(copies):
    for copy in copies:
        copy.wait()


def ff_rows(h1, gain, w1_s, w2_s, waits=None):
    xn = norm_rows(h1, gain)
    acc = None
    for c in range(FF // D):
        cols = slice(c * D, (c + 1) * D)
        second = c * D >= FF // 2
        if waits is not None and c in (0, FF // D // 2):
            wait_all(waits[2 * second])
        act = gelu(dot(xn, w1_s[:, cols])).astype(jnp.bfloat16)
        if waits is not None and c in (0, FF // D // 2):
            wait_all(waits[2 * second + 1])
        term = dot(act, w2_s[cols, :])
        acc = term if acc is None else acc + term
    return (h1.astype(jnp.float32) + acc).astype(jnp.bfloat16)


def pack_kernel(cfg, *refs):
    ins, outs, sem = refs[:cfg['nin']], refs[cfg['nin']:-1], refs[-1]
    stage = lax.axis_index('stage')
    copies = []
    for out, parts in zip(outs, cfg['groups']):
        base = 0
        for slot, index in parts:
            ref = ins[slot]
            size = ref.shape[-2] // 4
            for c in range(ref.shape[-1] // HALF):
                src = ref.at[index + (pl.ds(pl.multiple_of(stage * size, size), size), pl.ds(c * HALF, HALF))]
                copies.append(pltpu.make_async_copy(src, out.at[pl.ds(base, size), :], sem))
                base += size
    start_all(copies)
    wait_all(copies)


def group_rows(sources, parts):
    return sum(sources[slot].shape[-2] * sources[slot].shape[-1] // (4 * HALF) for slot, _ in parts)


def run_pack(sources, groups):
    hbm = pl.BlockSpec(memory_space=pl.ANY)
    vm = pl.BlockSpec(memory_space=pltpu.VMEM)
    shapes = [jax.ShapeDtypeStruct((group_rows(sources, parts), HALF), jnp.bfloat16) for parts in groups]
    return pl.pallas_call(
        functools.partial(pack_kernel, dict(nin=len(sources), groups=groups)),
        out_shape=shapes,
        in_specs=[hbm] * len(sources),
        out_specs=[vm] * len(groups),
        scratch_shapes=[pltpu.SemaphoreType.DMA],
        compiler_params=pltpu.CompilerParams(vmem_limit_bytes=VMEM_LIMIT),
        cost_estimate=pl.CostEstimate(flops=0, bytes_accessed=sum(4 * shape.size for shape in shapes), transcendentals=0),
    )(*sources)


def rows_at(i, size):
    return pl.ds(pl.multiple_of(i * size, size), size)


def project(h_ref, gain, w_s, cols, first, count, tile, dests, npair):
    def body(i, carry):
        rows = rows_at(first // tile + i, tile)
        x = h_ref[rows, :] if gain is None else norm_rows(h_ref[rows, :], gain)
        value = dot(x, w_s[:, cols])
        for d, dst in enumerate(dests):
            for pair in range(npair):
                col = (d * npair + pair) * LANES
                dst[pair, rows, :] = value[:, col:col + LANES].astype(jnp.bfloat16)
        return carry

    lax.fori_loop(0, count // tile, body, 0)


def attention(job, pairs, src_len, off_a, off_b, model_idx, q_s, k_s, v_s, km_s, vx_s, ctx_s):
    tq, tk, chunk_plan = job['tq'], job['tk'], job['chunks']
    causal = chunk_plan is not None
    qb = LANES
    npair = pairs
    lane = lax.broadcasted_iota(jnp.int32, (1, LANES), 1)
    lo_f = jnp.where(lane < HEAD_DIM, 1.0, 0.0).astype(jnp.float32)
    masks_f = (lo_f, 1.0 - lo_f)
    masks_b = [mask.astype(jnp.bfloat16) for mask in masks_f]
    nchunk = tk // CHUNK

    def pair_body(pair, carry):
        if not causal:
            k_first = jnp.where(off_a == 0, k_s[pair, 0:SUB, :].astype(jnp.float32)[0:1],
                                k_s[pair, HALF:HALF + SUB, :].astype(jnp.float32)[0:1])
        for c in range(nchunk):
            rows = slice(c * CHUNK, (c + 1) * CHUNK)
            v_f = v_s[pair, rows, :].astype(jnp.float32)
            ones = jnp.ones((CHUNK, LANES), jnp.float32)
            if not causal:
                idx = lax.broadcasted_iota(jnp.int32, (CHUNK, LANES), 0) + c * CHUNK
                pos = jnp.where(idx < HALF, idx + off_a, idx + (off_b - HALF))
                ok = pos < src_len
                km_s[rows, :] = jnp.where(ok, k_s[pair, rows, :].astype(jnp.float32), k_first).astype(jnp.bfloat16)
                v_f = jnp.where(ok, v_f, 0.0)
                ones = jnp.where(ok, ones, 0.0)
            for head, mask in enumerate(masks_f):
                vrows = slice((2 * c + head) * CHUNK, (2 * c + head + 1) * CHUNK)
                vx_s[vrows, :LANES] = (v_f * mask).astype(jnp.bfloat16)
                vx_s[vrows, LANES:] = (ones * mask).astype(jnp.bfloat16)
        for b in range(tq // qb):
            rows = slice(b * qb, (b + 1) * qb)
            qp = q_s[pair, rows, :]
            q2 = jnp.concatenate([qp * mask for mask in masks_b], axis=0)
            chunks, masks = chunk_plan[b * qb // CHUNK] if causal else (list(range(nchunk)), {})
            parts = []
            for start, count in runs_of(chunks):
                krows = slice(start * CHUNK, (start + count) * CHUNK)
                s_run = dot_t(q2, k_s[pair, krows, :] if causal else km_s[krows, :])
                for j in range(count):
                    s_c = s_run[:, j * CHUNK:(j + 1) * CHUNK]
                    kind = masks.get(start + j)
                    if kind == 'diag':
                        q_idx = lax.broadcasted_iota(jnp.int32, (2 * qb, CHUNK), 0)
                        q_idx = jnp.where(q_idx < qb, q_idx, q_idx - qb) + (b * qb % CHUNK)
                        k_idx = lax.broadcasted_iota(jnp.int32, (2 * qb, CHUNK), 1)
                        s_c = jnp.where(k_idx <= q_idx, s_c, NEG_BIG)
                    elif kind is not None:
                        s_c = jnp.where(model_idx == kind, s_c, NEG_BIG)
                    parts.append(s_c)
            top = functools.reduce(jnp.maximum, parts)
            top = jnp.max(top, axis=-1, keepdims=True)
            probs = [jnp.exp2((part - top) * EXP_SCALE).astype(jnp.bfloat16) for part in parts]
            terms = []
            for start, count in runs_of(chunks):
                used, probs = probs[:count], probs[count:]
                lhs = [half for prob in used for half in (prob[:qb], prob[qb:])]
                terms.append(dot(jnp.concatenate(lhs, axis=1), vx_s[2 * start * CHUNK:2 * (start + count) * CHUNK, :]))
            total = functools.reduce(jnp.add, terms)
            ctx_s[pair, rows, :] = (total[:, :LANES] / total[:, LANES:]).astype(jnp.bfloat16)
        return carry

    lax.fori_loop(0, npair, pair_body, 0)


def block_kernel(cfg, *refs):
    it = iter(refs)

    def take(n):
        return [next(it) for _ in range(n)]

    layer, kind, halves, ff, jobs = cfg['layer'], cfg['kind'], cfg['halves'], cfg['ff'], cfg['jobs']
    cross = kind == 'cross'
    nh = len(halves)
    npair, ncol = 3 * nh, HALF * nh
    lens, norm_in = take(2)
    final_in = take(1)[0] if cfg['final'] else None
    data = take(cfg['ndata'])
    own_refs = take(cfg['nown'])
    pieces = take(cfg['npiece'])
    if ff:
        w1_ref, w2_ref = take(2)
        up_pieces, down_pieces = take(4), take(4)
    outs = take(len(jobs))
    h_bufs = take(len(jobs))
    s_bufs = take(len(jobs)) if cross else None
    p_bufs = take(len(jobs)) if cfg['part_in'] else None
    o_bufs = take(len(jobs))
    if kind:
        w_s, wo_s, q_s, k_s, v_s, km_s, vx_s, ctx_s = take(8)
    if ff:
        w1_s, w2_s = take(2)
    norm_ref = take(1)[0]
    final_ref = take(1)[0] if cfg['final'] else None
    sem, job_sem, out_sem = take(3)
    m, stage = lax.axis_index('model'), lax.axis_index('stage')

    def load(parts, dst, semaphore):
        copies, base = [], 0
        for slot, lead, size, steps in parts:
            for a, b in steps:
                start = pl.multiple_of((a + b * m) * size, size) if lead is not None else 0
                src = data[slot]
                if lead is not None:
                    src = src.at[lead[0] + lead[1] * m]
                copies += row_copies(src.at[pl.ds(start, size), :], dst.at[pl.ds(base, size), :], semaphore, LANES)
                base += size
        return copies

    job_copies = []
    for j, job in enumerate(jobs):
        copies = load(job['h'], h_bufs[j], job_sem.at[j])
        if cross:
            copies += load(job['src'], s_bufs[j], job_sem.at[j])
        if cfg['part_in']:
            copies += load(job['part'], p_bufs[j], job_sem.at[j])
        job_copies.append(copies)
    job_copies[0].append(pltpu.make_async_copy(norm_in, norm_ref, job_sem.at[0]))
    if final_ref is not None:
        job_copies[0].append(pltpu.make_async_copy(final_in, final_ref, job_sem.at[0]))
    start_all(job_copies[0])
    qkv_copies, wo_copies, ff_groups = [], [], []
    if kind:
        if cross and own_refs:
            own = [own_refs[0].at[layer], own_refs[1].at[layer, 0], own_refs[1].at[layer, 1], own_refs[2].at[layer]]
        elif own_refs:
            own = [own_refs[0].at[layer, c] for c in range(3)] + [own_refs[1].at[layer]]
        else:
            own = []
        qkv_copies, wo_copies = attn_weight_copies(stage, own, pieces, cfg['base'], halves, w_s, wo_s, [sem.at[0], sem.at[1]])
        start_all(qkv_copies + wo_copies)
    for copies in job_copies[1:]:
        start_all(copies)
    if ff:
        ff_groups = ff_weight_copies(layer, stage, w1_ref, w2_ref, up_pieces, down_pieces, cfg['down_base'], w1_s, w2_s,
                                     [sem.at[2 + i] for i in range(4)])
        if not kind:
            for group in ff_groups:
                start_all(group)

    wait_all(job_copies[0])
    gain = norm_ref[layer, cfg['gain']][None, :]
    gain_f = norm_ref[layer, cfg['ff_gain']][None, :]
    for j, job in enumerate(jobs):
        tq, tk = job['tq'], job['tk']
        tile = TILE if tq % TILE == 0 else HALF
        h_ref, o_ref, out = h_bufs[j], o_bufs[j], outs[j]
        if j > 0:
            wait_all(job_copies[j])
        if kind:
            if j == 0:
                wait_all(qkv_copies)
                for group in ff_groups:
                    start_all(group)
            if cross:
                project(h_ref, gain, w_s, slice(0, ncol), 0, tq, tile, [q_s], npair)
                project(s_bufs[j], None, w_s, slice(ncol, 3 * ncol), 0, tk, TILE, [k_s, v_s], npair)
            else:
                project(h_ref, gain, w_s, slice(0, 3 * ncol), 0, tq, tile, [q_s, k_s, v_s], npair)
                if tk > tq:
                    project(h_ref, gain, w_s, slice(ncol, 3 * ncol), tq, tk - tq, tile, [k_s, v_s], npair)
            if job['full']:
                attention(job, npair, lens[2 * m], 0, HALF, m, q_s, k_s, v_s, km_s, vx_s, ctx_s)
            else:
                attention(job, npair, lens[1], HALF * m, HALF * (1 - m), m, q_s, k_s, v_s, km_s, vx_s, ctx_s)
            if j == 0:
                wait_all(wo_copies)
        if ff and kind and j == 0:
            for group in ff_groups:
                wait_all(group)

        def finish(rows, value, o_ref=o_ref, out=out):
            if final_ref is not None:
                value = norm_rows(value, final_ref[...][None, :])
            o_ref[rows, :] = value
            pltpu.make_async_copy(o_ref.at[rows, :], out.at[rows, :], out_sem).start()

        def out_tile(i, carry, h_ref=h_ref, tile=tile, finish=finish, j=j):
            rows = rows_at(i, tile)
            h1 = h_ref[rows, :]
            if kind:
                ctx = jnp.concatenate([ctx_s[pair, rows, :] for pair in range(npair)], axis=1)
                update = dot(ctx, wo_s[...])
                if cfg['part_in']:
                    update = update + p_bufs[j][rows, :]
                if cfg['part_out']:
                    finish(rows, update)
                    return carry
                h1 = (h1.astype(jnp.float32) + update).astype(jnp.bfloat16)
            if ff:
                h1 = ff_rows(h1, gain_f, w1_s, w2_s)
            finish(rows, h1)
            return carry

        first = 0
        if ff and not kind and j == 0:
            finish(pl.ds(0, tile), ff_rows(h_ref[:tile, :], gain_f, w1_s, w2_s, ff_groups))
            first = 1
        if tq // tile > first:
            lax.fori_loop(first, tq // tile, out_tile, 0)
    for j in range(len(jobs)):
        pltpu.make_async_copy(o_bufs[j], outs[j], out_sem).wait()


FULL_CHUNKS = [(list(range(i + 1)), {i: 'diag'}) for i in range(4)]
MID_CHUNKS = [([0, 2], {0: 'diag', 2: 1}), ([0, 1, 2, 3], {1: 'diag', 3: 0})]


def run_block(lens, norms, layer, kind, jobs, data, *, gain=0, ff_gain=0, own=(), pieces=(), base=0, part_in=False, part_out=False,
              ff=None, down_base=0, final_gain=None):
    halves = ((0,) if own else ()) + ((1,) if pieces else ())
    nh, bf = len(halves), jnp.bfloat16
    npair = 3 * nh
    cfg = dict(layer=layer, kind=kind, halves=halves, ff=ff is not None, jobs=jobs, ndata=len(data), nown=len(own), npiece=len(pieces),
               base=base, down_base=down_base, gain=gain, ff_gain=ff_gain, part_in=part_in, part_out=part_out, final=final_gain is not None)
    hbm = pl.BlockSpec(memory_space=pl.ANY)
    head = [norms] + ([final_gain] if final_gain is not None else [])
    rest = head + list(data) + list(own) + list(pieces)
    if ff is not None:
        rest += [ff[0], ff[1]] + list(ff[2]) + list(ff[3])
    odt = jnp.float32 if part_out else bf
    tq, tk = max(job['tq'] for job in jobs), max(job['tk'] for job in jobs)
    scratch = [pltpu.VMEM((job['tk'] if kind == 'self' else job['tq'], D), bf) for job in jobs]
    if kind == 'cross':
        scratch += [pltpu.VMEM((job['tk'], D), bf) for job in jobs]
    if part_in:
        scratch += [pltpu.VMEM((job['tq'], D), jnp.float32) for job in jobs]
    scratch += [pltpu.VMEM((job['tq'], D), odt) for job in jobs]
    if kind:
        scratch += [pltpu.VMEM(shape, bf) for shape in [
            (D, npair * LANES * 3), (HALF * nh, D), (npair, tq, LANES), (npair, tk, LANES), (npair, tk, LANES),
            (tk, LANES), (2 * tk, 2 * LANES), (npair, tq, LANES)]]
    if ff is not None:
        scratch += [pltpu.VMEM((D, FF), bf), pltpu.VMEM((FF, D), bf)]
    scratch += [pltpu.VMEM(value.shape, jnp.float32) for value in head]
    scratch += [pltpu.SemaphoreType.DMA((6,)), pltpu.SemaphoreType.DMA((2,)), pltpu.SemaphoreType.DMA]
    scores = sum(job['tq'] * job['tk'] * npair * 2 for job in jobs)
    rows_q = sum(job['tq'] for job in jobs)
    flops = scores * 512 + 8 * D * HALF * nh * rows_q + (4 * D * FF * rows_q if ff is not None else 0)
    nbytes = 4 * D * rows_q + 8 * D * HALF * nh + (4 * D * FF if ff is not None else 0)
    return pl.pallas_call(
        functools.partial(block_kernel, cfg),
        out_shape=[jax.ShapeDtypeStruct((job['tq'], D), odt) for job in jobs],
        in_specs=[pl.BlockSpec(memory_space=pltpu.SMEM)] + [hbm] * len(rest),
        out_specs=[hbm] * len(jobs),
        scratch_shapes=scratch,
        compiler_params=pltpu.CompilerParams(vmem_limit_bytes=VMEM_LIMIT),
        cost_estimate=pl.CostEstimate(flops=flops, bytes_accessed=nbytes, transcendentals=scores),
    )(lens, *rest)


def solution(mesh):
    row_spec = P(('data', 'stage'), None, None)
    len_spec = P(('data', 'stage'))
    qkv_spec = P(None, None, None, 'model')
    col_spec = P(None, None, 'model')
    row_w_spec = P(None, 'model', None)
    rep_spec = P()
    in_specs_all = (row_spec, len_spec, row_spec, qkv_spec, row_w_spec, col_spec, row_w_spec, rep_spec, rep_spec,
                    qkv_spec, row_w_spec, col_spec, qkv_spec, row_w_spec, col_spec, row_w_spec, rep_spec)
    perms = dict(y=('model', [(0, 1), (1, 0)]), x=('stage', [(i, i ^ 2) for i in range(4)]), c=('stage', [(i, i ^ 1) for i in range(4)]))

    def permute(kind, value):
        return lax.ppermute(value, *perms[kind])

    def spread(pack):
        first = permute('y', pack)
        second = permute('x', first)
        return [first, second, permute('c', first), permute('c', second)]

    def local_step(x_enc, enc_len, y_dec, enc_wqkv, enc_wo, enc_w1, enc_w2, enc_norm, enc_final,
                   dec_wqkv, dec_wo, crs_wq, crs_wkv, crs_wo, dec_w1, dec_w2, dec_norm):
        src, tgt = x_enc.shape[1], y_dec.shape[1]
        enc_qkv_t, dec_qkv_t, crs_kv_t = [jnp.transpose(w, (0, 2, 1, 3)) for w in (enc_wqkv, dec_wqkv, crs_wkv)]
        pair_len = permute('x', enc_len)

        sources_a = [enc_qkv_t, enc_wo, enc_w1, enc_w2, dec_qkv_t, dec_wo]
        sources_b = sources_a + [crs_wq, crs_kv_t, crs_wo, dec_w1, dec_w2]

        def self_parts(slot, layer):
            return [(slot, (layer, c)) for c in range(3)] + [(slot + 1, (layer,))]

        def cross_parts(layer):
            return [(6, (layer,))] + [(7, (layer, c)) for c in range(2)] + [(8, (layer,))]

        def one(slot, layer):
            return [(slot, (layer,))]

        groups_a = [self_parts(0, 0), one(2, 0) + one(3, 0), self_parts(4, 0)]
        groups_b = [self_parts(0, 1), one(2, 1) + one(3, 1), cross_parts(0), one(9, 0) + one(10, 0),
                    self_parts(4, 1) + cross_parts(1), one(9, 1) + one(10, 1)]
        packs = list(run_pack(sources_a, groups_a))
        packs += list(run_pack(sources_b, groups_b))
        w = [spread(pack) for pack in packs]

        full_lead, mid_lead = (0, 2), (1, 0)
        same = [(0, 0)]

        def job(full, tq, tk, h, chunks=None, **extra):
            return dict(full=full, tq=tq, tk=tk, h=h, chunks=chunks, **extra)

        def flat(*slots_sizes):
            return [(slot, None, size, same) for slot, size in slots_sizes]

        hs, ht = src // 2, tgt // 2
        x_mid = [(0, mid_lead, hs, [(0, 1), (1, -1)])]
        x_full = [(0, full_lead, src, same)]
        y_mid = [(0, mid_lead, CHUNK, [(0, 1), (3, -1), (1, -1), (2, 1)])]
        y_full = [(0, full_lead, tgt, same)]
        e_own, d_own, c_own = (enc_qkv_t, enc_wo), (dec_qkv_t, dec_wo), (crs_wq, crs_kv_t, crs_wo)

        pd_mid, pd_full = run_block(enc_len, dec_norm, 0, 'self', [job(False, ht, tgt, y_mid, MID_CHUNKS), job(True, tgt, tgt, y_full, FULL_CHUNKS)],
                                [y_dec], own=d_own, part_out=True)
        pe_mid, pe_full = run_block(enc_len, enc_norm, 0, 'self', [job(False, hs, src, x_mid), job(True, src, src, x_full)],
                                [x_enc], own=e_own, part_out=True)
        h_mid, h_full = run_block(enc_len, enc_norm, 0, 'self',
                              [job(False, hs, src, x_mid, part=flat((1, hs))), job(True, src, src, x_full, part=flat((2, src)))],
                              [x_enc, pe_mid, pe_full], pieces=w[0], part_in=True)
        h_mid, h_full = run_block(enc_len, enc_norm, 0, '', [job(False, hs, hs, flat((0, hs))), job(True, src, src, flat((1, src)))],
                              [h_mid, h_full], ff_gain=1, ff=(enc_w1, enc_w2, w[1], w[1]), down_base=D)
        h_other = permute('y', h_mid)
        z_mid, = run_block(enc_len, dec_norm, 0, 'self', [job(False, ht, tgt, y_mid, MID_CHUNKS, part=flat((1, ht)))],
                       [y_dec, pd_mid], pieces=w[2], part_in=True)
        e1 = dict(own=e_own, pieces=w[3], ff_gain=1, ff=(enc_w1, enc_w2, w[4], w[4]), down_base=D, final_gain=enc_final)
        s_mid, = run_block(enc_len, enc_norm, 1, 'self', [job(False, hs, src, flat((0, hs), (1, hs)))], [h_mid, h_other], **e1)
        s_mid = permute('x', s_mid)
        s_full, = run_block(enc_len, enc_norm, 1, 'self', [job(True, src, src, flat((0, src)))], [h_full], **e1)
        s_other = permute('y', s_mid)
        s_full = permute('x', s_full)
        z_full, = run_block(enc_len, dec_norm, 0, 'self', [job(True, tgt, tgt, y_full, FULL_CHUNKS, part=flat((1, tgt)))],
                        [y_dec, pd_full], pieces=w[2], part_in=True)

        def cross_mid(z, layer, **kwargs):
            return run_block(pair_len, dec_norm, layer, 'cross', [job(False, ht, src, flat((0, ht)), src=flat((1, hs), (2, hs)))],
                         [z, s_mid, s_other], own=c_own, gain=1, ff_gain=2, **kwargs)[0]

        def cross_full(z, layer, **kwargs):
            return run_block(pair_len, dec_norm, layer, 'cross', [job(True, tgt, src, flat((0, tgt)), src=flat((1, src)))],
                         [z, s_full], own=c_own, gain=1, ff_gain=2, **kwargs)[0]

        cross0 = dict(pieces=w[5], ff=(dec_w1, dec_w2, w[6], w[6]), down_base=D)
        cross1 = dict(pieces=w[7], base=D, ff=(dec_w1, dec_w2, w[8], w[8]), down_base=D)
        z_mid = cross_mid(z_mid, 0, **cross0)
        z_other = permute('y', z_mid)
        z_full = cross_full(z_full, 0, **cross0)
        z_full, = run_block(enc_len, dec_norm, 1, 'self', [job(True, tgt, tgt, flat((0, tgt)), FULL_CHUNKS)], [z_full], own=d_own, pieces=w[7])
        z_full = cross_full(z_full, 1, **cross1)
        z_full_other = permute('y', z_full)
        z_mid, = run_block(enc_len, dec_norm, 1, 'self', [job(False, ht, tgt, flat((0, ht), (1, ht)), MID_CHUNKS)], [z_mid, z_other],
                       own=d_own, pieces=w[7])
        z_mid = cross_mid(z_mid, 1, **cross1)
        z_mid_other = permute('y', z_mid)

        first = lax.axis_index('model') == 0
        a, b, oa, ob = z_mid[:CHUNK], z_mid[CHUNK:], z_mid_other[:CHUNK], z_mid_other[CHUNK:]
        row_mid = jnp.where(first, jnp.concatenate([a, oa, ob, b], axis=0), jnp.concatenate([oa, a, b, ob], axis=0))
        return jnp.stack([jnp.where(first, z_full, z_full_other), row_mid, jnp.where(first, z_full_other, z_full)])

    return jax.shard_map(local_step, mesh=mesh, in_specs=in_specs_all, out_specs=row_spec, check_vma=False)
```

```python
import functools
import math

import jax
import jax.numpy as jnp
from jax import lax
from jax.experimental import pallas as pl
from jax.experimental.pallas import tpu as pltpu
from jax.sharding import PartitionSpec as P


D = 768
HALF = 384
FF = 3072
NORM_EPS = 1e-6
NEG_BIG = -1e30
EXP_SCALE = 0.125 * math.log2(math.e)
GELU_C = math.sqrt(2.0 / math.pi)
PIECE_XOR = (0, 2, 1, 3)
QROWS = 192
OROWS = 96
TILE = 256
CHUNK = 256
LANES = 128
SUB = 16
HEAD_DIM = 64
VMEM_LIMIT = 60 * 1024 * 1024


def norm_rows(h, gain):
    hf = h.astype(jnp.float32)
    inv = lax.rsqrt(jnp.mean(hf * hf, axis=-1, keepdims=True) + NORM_EPS)
    return (hf * inv * gain).astype(jnp.bfloat16)


def gelu(x):
    return x * (0.5 + 0.5 * jnp.tanh(GELU_C * (x + 0.044715 * (x * x * x))))


def dot(a, b):
    return jnp.dot(a, b, preferred_element_type=jnp.float32)


def dot_t(a, b):
    return lax.dot_general(a, b, (((1,), (1,)), ((), ())), preferred_element_type=jnp.float32)


def runs_of(chunks):
    runs = []
    for c in chunks:
        if runs and runs[-1][0] + runs[-1][1] == c:
            runs[-1] = (runs[-1][0], runs[-1][1] + 1)
        else:
            runs.append((c, 1))
    return runs


def row_copies(src, dst, sem, step):
    rows = src.shape[0]
    return [pltpu.make_async_copy(src.at[pl.ds(r, step), :], dst.at[pl.ds(r, step), :], sem) for r in range(0, rows, step)]


def attn_weight_copies(stage, own, pieces, base, halves, w_s, wo_s, sems):
    ncol = HALF * len(halves)
    off = ncol - HALF
    qkv, out = [], []
    if own:
        for c, src in enumerate(own[:-1]):
            qkv += row_copies(src, w_s.at[:, pl.ds(c * ncol, HALF)], sems[0], QROWS)
        out += row_copies(own[-1], wo_s.at[pl.ds(0, HALF), :], sems[1], OROWS)
    for piece, mask in zip(pieces, PIECE_XOR):
        quarter = stage ^ mask
        r0 = pl.multiple_of(quarter * QROWS, QROWS)
        for c in range(3):
            qkv.append(pltpu.make_async_copy(piece.at[pl.ds(base + c * QROWS, QROWS), :],
                                             w_s.at[pl.ds(r0, QROWS), pl.ds(c * ncol + off, HALF)], sems[0]))
        r1 = pl.multiple_of(off + quarter * OROWS, OROWS)
        for c in range(2):
            out.append(pltpu.make_async_copy(piece.at[pl.ds(base + 3 * QROWS + c * OROWS, OROWS), :],
                                             wo_s.at[pl.ds(r1, OROWS), pl.ds(c * HALF, HALF)], sems[1]))
    return qkv, out


def ff_weight_copies(layer, stage, w1_ref, w2_ref, up_pieces, down_pieces, down_base, w1_s, w2_s, sems):
    hf = FF // 2
    own_up = row_copies(w1_ref.at[layer], w1_s.at[:, pl.ds(0, hf)], sems[0], OROWS // 2)
    own_down = row_copies(w2_ref.at[layer], w2_s.at[pl.ds(0, hf), :], sems[1], OROWS)
    up, down = [], []
    for i, mask in enumerate(PIECE_XOR):
        quarter = stage ^ mask
        r0 = pl.multiple_of(quarter * QROWS, QROWS)
        for c in range(4):
            up.append(pltpu.make_async_copy(up_pieces[i].at[pl.ds(c * QROWS, QROWS), :],
                                            w1_s.at[pl.ds(r0, QROWS), pl.ds(hf + c * HALF, HALF)], sems[2]))
        r1 = pl.multiple_of(hf + quarter * HALF, HALF)
        for c in range(2):
            down.append(pltpu.make_async_copy(down_pieces[i].at[pl.ds(down_base + c * HALF, HALF), :],
                                              w2_s.at[pl.ds(r1, HALF), pl.ds(c * HALF, HALF)], sems[3]))
    return [own_up, own_down, up, down]


def start_all(copies):
    for copy in copies:
        copy.start()


def wait_all(copies):
    for copy in copies:
        copy.wait()


def ff_rows(h1, gain, w1_s, w2_s, waits=None):
    xn = norm_rows(h1, gain)
    acc = None
    for c in range(FF // D):
        cols = slice(c * D, (c + 1) * D)
        second = c * D >= FF // 2
        if waits is not None and c in (0, FF // D // 2):
            wait_all(waits[2 * second])
        act = gelu(dot(xn, w1_s[:, cols])).astype(jnp.bfloat16)
        if waits is not None and c in (0, FF // D // 2):
            wait_all(waits[2 * second + 1])
        term = dot(act, w2_s[cols, :])
        acc = term if acc is None else acc + term
    return (h1.astype(jnp.float32) + acc).astype(jnp.bfloat16)


def pack_kernel(cfg, *refs):
    ins, outs, sem = refs[:cfg['nin']], refs[cfg['nin']:-1], refs[-1]
    stage = lax.axis_index('stage')
    copies = []
    for out, parts in zip(outs, cfg['groups']):
        base = 0
        for slot, index in parts:
            ref = ins[slot]
            size = ref.shape[-2] // 4
            for c in range(ref.shape[-1] // HALF):
                src = ref.at[index + (pl.ds(pl.multiple_of(stage * size, size), size), pl.ds(c * HALF, HALF))]
                copies.append(pltpu.make_async_copy(src, out.at[pl.ds(base, size), :], sem))
                base += size
    if cfg['row'] is not None:
        copies += row_copies(ins[cfg['row']].at[2 * lax.axis_index('model')], outs[-1], sem, LANES)
    start_all(copies)
    wait_all(copies)


def group_rows(sources, parts):
    return sum(sources[slot].shape[-2] * sources[slot].shape[-1] // (4 * HALF) for slot, _ in parts)


def run_pack(sources, groups, row=None):
    hbm = pl.BlockSpec(memory_space=pl.ANY)
    vm = pl.BlockSpec(memory_space=pltpu.VMEM)
    shapes = [jax.ShapeDtypeStruct((group_rows(sources, parts), HALF), jnp.bfloat16) for parts in groups]
    if row is not None:
        shapes.append(jax.ShapeDtypeStruct(sources[row].shape[1:], jnp.bfloat16))
    return pl.pallas_call(
        functools.partial(pack_kernel, dict(nin=len(sources), groups=groups, row=row)),
        out_shape=shapes,
        in_specs=[hbm] * len(sources),
        out_specs=[vm] * len(shapes),
        scratch_shapes=[pltpu.SemaphoreType.DMA],
        compiler_params=pltpu.CompilerParams(vmem_limit_bytes=VMEM_LIMIT),
        cost_estimate=pl.CostEstimate(flops=0, bytes_accessed=sum(4 * shape.size for shape in shapes), transcendentals=0),
    )(*sources)


def rows_at(i, size):
    return pl.ds(pl.multiple_of(i * size, size), size)


def project(h_ref, gain, w_s, cols, first, count, tile, dests, npair):
    def body(i, carry):
        rows = rows_at(first // tile + i, tile)
        x = h_ref[rows, :] if gain is None else norm_rows(h_ref[rows, :], gain)
        value = dot(x, w_s[:, cols])
        for d, dst in enumerate(dests):
            for pair in range(npair):
                col = (d * npair + pair) * LANES
                dst[pair, rows, :] = value[:, col:col + LANES].astype(jnp.bfloat16)
        return carry

    lax.fori_loop(0, count // tile, body, 0)


def attention(job, pairs, src_len, off_a, off_b, model_idx, q_s, k_s, v_s, km_s, vx_s, ctx_s):
    tq, tk, chunk_plan = job['tq'], job['tk'], job['chunks']
    causal = chunk_plan is not None
    qb = job['qb']
    npair = pairs
    lane = lax.broadcasted_iota(jnp.int32, (1, LANES), 1)
    lo_f = jnp.where(lane < HEAD_DIM, 1.0, 0.0).astype(jnp.float32)
    masks_f = (lo_f, 1.0 - lo_f)
    masks_b = [mask.astype(jnp.bfloat16) for mask in masks_f]
    nchunk = tk // CHUNK

    def pair_body(pair, carry):
        if not causal:
            k_first = jnp.where(off_a == 0, k_s[pair, 0:SUB, :].astype(jnp.float32)[0:1],
                                k_s[pair, HALF:HALF + SUB, :].astype(jnp.float32)[0:1])
        for c in range(nchunk):
            rows = slice(c * CHUNK, (c + 1) * CHUNK)
            v_f = v_s[pair, rows, :].astype(jnp.float32)
            ones = jnp.ones((CHUNK, LANES), jnp.float32)
            if not causal:
                idx = lax.broadcasted_iota(jnp.int32, (CHUNK, LANES), 0) + c * CHUNK
                pos = jnp.where(idx < HALF, idx + off_a, idx + (off_b - HALF))
                ok = pos < src_len
                km_s[rows, :] = jnp.where(ok, k_s[pair, rows, :].astype(jnp.float32), k_first).astype(jnp.bfloat16)
                v_f = jnp.where(ok, v_f, 0.0)
                ones = jnp.where(ok, ones, 0.0)
            for head, mask in enumerate(masks_f):
                vrows = slice((2 * c + head) * CHUNK, (2 * c + head + 1) * CHUNK)
                vx_s[vrows, :LANES] = (v_f * mask).astype(jnp.bfloat16)
                vx_s[vrows, LANES:] = (ones * mask).astype(jnp.bfloat16)
        for b in range(tq // qb):
            rows = slice(b * qb, (b + 1) * qb)
            qp = q_s[pair, rows, :]
            q2 = jnp.concatenate([qp * mask for mask in masks_b], axis=0)
            chunks, masks = chunk_plan[b * qb // CHUNK] if causal else (list(range(nchunk)), {})
            parts = []
            for start, count in runs_of(chunks):
                krows = slice(start * CHUNK, (start + count) * CHUNK)
                s_run = dot_t(q2, k_s[pair, krows, :] if causal else km_s[krows, :])
                for j in range(count):
                    s_c = s_run[:, j * CHUNK:(j + 1) * CHUNK]
                    kind = masks.get(start + j)
                    if kind == 'diag':
                        q_idx = lax.broadcasted_iota(jnp.int32, (2 * qb, CHUNK), 0)
                        q_idx = jnp.where(q_idx < qb, q_idx, q_idx - qb) + (b * qb % CHUNK)
                        k_idx = lax.broadcasted_iota(jnp.int32, (2 * qb, CHUNK), 1)
                        s_c = jnp.where(k_idx <= q_idx, s_c, NEG_BIG)
                    elif kind is not None:
                        s_c = jnp.where(model_idx == kind, s_c, NEG_BIG)
                    parts.append(s_c)
            top = functools.reduce(jnp.maximum, parts)
            top = jnp.max(top, axis=-1, keepdims=True)
            probs = [jnp.exp2((part - top) * EXP_SCALE).astype(jnp.bfloat16) for part in parts]
            terms = []
            for start, count in runs_of(chunks):
                used, probs = probs[:count], probs[count:]
                lhs = [half for prob in used for half in (prob[:qb], prob[qb:])]
                terms.append(dot(jnp.concatenate(lhs, axis=1), vx_s[2 * start * CHUNK:2 * (start + count) * CHUNK, :]))
            total = functools.reduce(jnp.add, terms)
            ctx_s[pair, rows, :] = (total[:, :LANES] / total[:, LANES:]).astype(jnp.bfloat16)
        return carry

    lax.fori_loop(0, npair, pair_body, 0)


def block_kernel(cfg, *refs):
    it = iter(refs)

    def take(n):
        return [next(it) for _ in range(n)]

    layer, kind, halves, ff, jobs = cfg['layer'], cfg['kind'], cfg['halves'], cfg['ff'], cfg['jobs']
    cross = kind == 'cross'
    nh = len(halves)
    npair, ncol = 3 * nh, HALF * nh
    lens_mid, lens_full, norm_in = take(3)
    final_in = take(1)[0] if cfg['final'] else None
    data = take(cfg['ndata'])
    own_refs = take(cfg['nown'])
    pieces = take(cfg['npiece'])
    if ff:
        w1_ref, w2_ref = take(2)
        up_pieces, down_pieces = take(4), take(4)
    outs = take(len(jobs))
    h_bufs = take(len(jobs))
    s_bufs = take(len(jobs)) if cross else None
    p_bufs = take(len(jobs)) if cfg['part_in'] else None
    o_bufs = take(len(jobs))
    if kind:
        w_s, wo_s, q_s, k_s, v_s, km_s, vx_s, ctx_s = take(8)
    if ff:
        w1_s, w2_s = take(2)
    norm_ref = take(1)[0]
    final_ref = take(1)[0] if cfg['final'] else None
    sem, job_sem, out_sem = take(3)
    m, stage = lax.axis_index('model'), lax.axis_index('stage')

    def load(parts, dst, semaphore):
        copies, base = [], 0
        for slot, lead, size, steps in parts:
            for a, b in steps:
                start = pl.multiple_of((a + b * m) * size, size) if lead is not None else 0
                src = data[slot]
                if lead is not None:
                    src = src.at[lead[0] + lead[1] * m]
                copies += row_copies(src.at[pl.ds(start, size), :], dst.at[pl.ds(base, size), :], semaphore, LANES)
                base += size
        return copies

    job_copies = []
    for j, job in enumerate(jobs):
        copies = load(job['h'], h_bufs[j], job_sem.at[j])
        if cross:
            copies += load(job['src'], s_bufs[j], job_sem.at[j])
        if cfg['part_in']:
            copies += load(job['part'], p_bufs[j], job_sem.at[j])
        job_copies.append(copies)
    job_copies[0].append(pltpu.make_async_copy(norm_in, norm_ref, job_sem.at[0]))
    if final_ref is not None:
        job_copies[0].append(pltpu.make_async_copy(final_in, final_ref, job_sem.at[0]))
    start_all(job_copies[0])
    qkv_copies, wo_copies, ff_groups = [], [], []
    if kind:
        if cross and own_refs:
            own = [own_refs[0].at[layer], own_refs[1].at[layer, 0], own_refs[1].at[layer, 1], own_refs[2].at[layer]]
        elif own_refs:
            own = [own_refs[0].at[layer, c] for c in range(3)] + [own_refs[1].at[layer]]
        else:
            own = []
        qkv_copies, wo_copies = attn_weight_copies(stage, own, pieces, cfg['base'], halves, w_s, wo_s, [sem.at[0], sem.at[1]])
        start_all(qkv_copies + wo_copies)
    for copies in job_copies[1:]:
        start_all(copies)
    if ff:
        ff_groups = ff_weight_copies(layer, stage, w1_ref, w2_ref, up_pieces, down_pieces, cfg['down_base'], w1_s, w2_s,
                                     [sem.at[2 + i] for i in range(4)])
        if not kind:
            for group in ff_groups:
                start_all(group)

    wait_all(job_copies[0])
    gain = norm_ref[layer, cfg['gain']][None, :]
    gain_f = norm_ref[layer, cfg['ff_gain']][None, :]
    for j, job in enumerate(jobs):
        tq, tk = job['tq'], job['tk']
        tile = TILE if tq % TILE == 0 else HALF
        h_ref, o_ref, out = h_bufs[j], o_bufs[j], outs[j]
        if j > 0:
            wait_all(job_copies[j])
        if kind:
            if j == 0:
                wait_all(qkv_copies)
                for group in ff_groups:
                    start_all(group)
            if cross:
                project(h_ref, gain, w_s, slice(0, ncol), 0, tq, tile, [q_s], npair)
                project(s_bufs[j], None, w_s, slice(ncol, 3 * ncol), 0, tk, TILE, [k_s, v_s], npair)
            else:
                project(h_ref, gain, w_s, slice(0, 3 * ncol), 0, tq, tile, [q_s, k_s, v_s], npair)
                if tk > tq:
                    project(h_ref, gain, w_s, slice(ncol, 3 * ncol), tq, tk - tq, tile, [k_s, v_s], npair)
            if job['full']:
                attention(job, npair, lens_full[2 * m], 0, HALF, m, q_s, k_s, v_s, km_s, vx_s, ctx_s)
            else:
                attention(job, npair, lens_mid[1], HALF * m, HALF * (1 - m), m, q_s, k_s, v_s, km_s, vx_s, ctx_s)
            if j == 0:
                wait_all(wo_copies)
        if ff and kind and j == 0:
            for group in ff_groups:
                wait_all(group)

        def finish(rows, value, o_ref=o_ref, out=out):
            if final_ref is not None:
                value = norm_rows(value, final_ref[...][None, :])
            o_ref[rows, :] = value
            pltpu.make_async_copy(o_ref.at[rows, :], out.at[rows, :], out_sem).start()

        def out_tile(i, carry, h_ref=h_ref, tile=tile, finish=finish, j=j):
            rows = rows_at(i, tile)
            h1 = h_ref[rows, :]
            if kind:
                ctx = jnp.concatenate([ctx_s[pair, rows, :] for pair in range(npair)], axis=1)
                update = dot(ctx, wo_s[...])
                if cfg['part_in']:
                    update = update + p_bufs[j][rows, :]
                if cfg['part_out']:
                    finish(rows, update)
                    return carry
                h1 = (h1.astype(jnp.float32) + update).astype(jnp.bfloat16)
            if ff:
                h1 = ff_rows(h1, gain_f, w1_s, w2_s)
            finish(rows, h1)
            return carry

        first = 0
        if ff and not kind and j == 0:
            finish(pl.ds(0, tile), ff_rows(h_ref[:tile, :], gain_f, w1_s, w2_s, ff_groups))
            first = 1
        if tq // tile > first:
            lax.fori_loop(first, tq // tile, out_tile, 0)
    for j in range(len(jobs)):
        pltpu.make_async_copy(o_bufs[j], outs[j], out_sem).wait()


FULL_CHUNKS = [(list(range(i + 1)), {i: 'diag'}) for i in range(4)]
MID_CHUNKS = [([0, 2], {0: 'diag', 2: 1}), ([0, 1, 2, 3], {1: 'diag', 3: 0})]


def run_block(lens, norms, layer, kind, jobs, data, *, gain=0, ff_gain=0, own=(), pieces=(), base=0, part_in=False, part_out=False,
              ff=None, down_base=0, final_gain=None):
    halves = ((0,) if own else ()) + ((1,) if pieces else ())
    nh, bf = len(halves), jnp.bfloat16
    npair = 3 * nh
    cfg = dict(layer=layer, kind=kind, halves=halves, ff=ff is not None, jobs=jobs, ndata=len(data), nown=len(own), npiece=len(pieces),
               base=base, down_base=down_base, gain=gain, ff_gain=ff_gain, part_in=part_in, part_out=part_out, final=final_gain is not None)
    hbm = pl.BlockSpec(memory_space=pl.ANY)
    head = [norms] + ([final_gain] if final_gain is not None else [])
    rest = head + list(data) + list(own) + list(pieces)
    if ff is not None:
        rest += [ff[0], ff[1]] + list(ff[2]) + list(ff[3])
    odt = jnp.float32 if part_out else bf
    tq, tk = max(job['tq'] for job in jobs), max(job['tk'] for job in jobs)
    scratch = [pltpu.VMEM((job['tk'] if kind == 'self' else job['tq'], D), bf) for job in jobs]
    if kind == 'cross':
        scratch += [pltpu.VMEM((job['tk'], D), bf) for job in jobs]
    if part_in:
        scratch += [pltpu.VMEM((job['tq'], D), jnp.float32) for job in jobs]
    scratch += [pltpu.VMEM((job['tq'], D), odt) for job in jobs]
    if kind:
        scratch += [pltpu.VMEM(shape, bf) for shape in [
            (D, npair * LANES * 3), (HALF * nh, D), (npair, tq, LANES), (npair, tk, LANES), (npair, tk, LANES),
            (tk, LANES), (2 * tk, 2 * LANES), (npair, tq, LANES)]]
    if ff is not None:
        scratch += [pltpu.VMEM((D, FF), bf), pltpu.VMEM((FF, D), bf)]
    scratch += [pltpu.VMEM(value.shape, jnp.float32) for value in head]
    scratch += [pltpu.SemaphoreType.DMA((6,)), pltpu.SemaphoreType.DMA((2,)), pltpu.SemaphoreType.DMA]
    scores = sum(job['tq'] * job['tk'] * npair * 2 for job in jobs)
    rows_q = sum(job['tq'] for job in jobs)
    flops = scores * 512 + 8 * D * HALF * nh * rows_q + (4 * D * FF * rows_q if ff is not None else 0)
    nbytes = 4 * D * rows_q + 8 * D * HALF * nh + (4 * D * FF if ff is not None else 0)
    return pl.pallas_call(
        functools.partial(block_kernel, cfg),
        out_shape=[jax.ShapeDtypeStruct((job['tq'], D), odt) for job in jobs],
        in_specs=[pl.BlockSpec(memory_space=pltpu.SMEM)] * 2 + [hbm] * len(rest),
        out_specs=[hbm] * len(jobs),
        scratch_shapes=scratch,
        compiler_params=pltpu.CompilerParams(vmem_limit_bytes=VMEM_LIMIT),
        cost_estimate=pl.CostEstimate(flops=flops, bytes_accessed=nbytes, transcendentals=scores),
    )(*lens, *rest)


def solution(mesh):
    row_spec = P(('data', 'stage'), None, None)
    len_spec = P(('data', 'stage'))
    qkv_spec = P(None, None, None, 'model')
    col_spec = P(None, None, 'model')
    row_w_spec = P(None, 'model', None)
    rep_spec = P()
    in_specs_all = (row_spec, len_spec, row_spec, qkv_spec, row_w_spec, col_spec, row_w_spec, rep_spec, rep_spec,
                    qkv_spec, row_w_spec, col_spec, qkv_spec, row_w_spec, col_spec, row_w_spec, rep_spec)
    perms = dict(y=('model', [(0, 1), (1, 0)]), x=('stage', [(i, i ^ 2) for i in range(4)]), c=('stage', [(i, i ^ 1) for i in range(4)]))

    def permute(kind, value):
        return lax.ppermute(value, *perms[kind])

    def spread(pack):
        first = permute('y', pack)
        second = permute('x', first)
        return [first, second, permute('c', first), permute('c', second)]

    def local_step(x_enc, enc_len, y_dec, enc_wqkv, enc_wo, enc_w1, enc_w2, enc_norm, enc_final,
                   dec_wqkv, dec_wo, crs_wq, crs_wkv, crs_wo, dec_w1, dec_w2, dec_norm):
        src, tgt = x_enc.shape[1], y_dec.shape[1]
        enc_qkv_t, dec_qkv_t, crs_kv_t = [jnp.transpose(w, (0, 2, 1, 3)) for w in (enc_wqkv, dec_wqkv, crs_wkv)]
        pair_len = permute('x', enc_len)
        own_len = (enc_len, pair_len)

        sources_a = [enc_qkv_t, enc_wo, enc_w1, enc_w2, dec_qkv_t, dec_wo]
        sources_b = sources_a + [crs_wq, crs_kv_t, crs_wo, dec_w1, dec_w2]

        def self_parts(slot, layer):
            return [(slot, (layer, c)) for c in range(3)] + [(slot + 1, (layer,))]

        def cross_parts(layer):
            return [(6, (layer,))] + [(7, (layer, c)) for c in range(2)] + [(8, (layer,))]

        def one(slot, layer):
            return [(slot, (layer,))]

        groups_a = [self_parts(0, 0), one(2, 0) + one(3, 0)]
        groups_b = [self_parts(0, 1), one(2, 1) + one(3, 1), self_parts(4, 0), cross_parts(0), one(9, 0) + one(10, 0),
                    self_parts(4, 1) + cross_parts(1), one(9, 1) + one(10, 1)]
        *packs, x_row = run_pack(sources_a[:4] + [x_enc], groups_a, row=4)
        packs += list(run_pack(sources_b, groups_b))
        x_row = permute('x', x_row)
        w = [spread(pack) for pack in packs]

        full_lead, mid_lead = (0, 2), (1, 0)
        same = [(0, 0)]

        def job(full, tq, tk, h, chunks=None, **extra):
            return dict(full=full, tq=tq, tk=tk, h=h, chunks=chunks, qb=LANES, **extra)

        def flat(*slots_sizes):
            return [(slot, None, size, same) for slot, size in slots_sizes]

        hs, ht = src // 2, tgt // 2
        x_mid = [(0, mid_lead, hs, [(0, 1), (1, -1)])]
        y_mid = [(0, mid_lead, CHUNK, [(0, 1), (3, -1), (1, -1), (2, 1)])]
        y_full = [(0, full_lead, tgt, same)]
        e_own, d_own, c_own = (enc_qkv_t, enc_wo), (dec_qkv_t, dec_wo), (crs_wq, crs_kv_t, crs_wo)

        pd_mid, pd_full = run_block(own_len, dec_norm, 0, 'self', [job(False, ht, tgt, y_mid, MID_CHUNKS), job(True, tgt, tgt, y_full, FULL_CHUNKS)],
                                [y_dec], own=d_own, part_out=True)
        pe_mid, pe_full = run_block(own_len, enc_norm, 0, 'self', [job(False, hs, src, x_mid), job(True, src, src, flat((1, src)))],
                                [x_enc, x_row], own=e_own, part_out=True)
        h_mid, h_full = run_block(own_len, enc_norm, 0, 'self',
                              [job(False, hs, src, x_mid, part=flat((2, hs))), job(True, src, src, flat((1, src)), part=flat((3, src)))],
                              [x_enc, x_row, pe_mid, pe_full], pieces=w[0], part_in=True)
        h_mid, h_full = run_block(own_len, enc_norm, 0, '', [job(False, hs, hs, flat((0, hs))), job(True, src, src, flat((1, src)))],
                              [h_mid, h_full], ff_gain=1, ff=(enc_w1, enc_w2, w[1], w[1]), down_base=D)
        h_other = permute('y', h_mid)
        z_mid, = run_block(own_len, dec_norm, 0, 'self', [job(False, ht, tgt, y_mid, MID_CHUNKS, part=flat((1, ht)))],
                       [y_dec, pd_mid], pieces=w[4], part_in=True)
        e1 = dict(own=e_own, pieces=w[2], ff_gain=1, ff=(enc_w1, enc_w2, w[3], w[3]), down_base=D, final_gain=enc_final)
        s_mid, = run_block(own_len, enc_norm, 1, 'self', [job(False, hs, src, flat((0, hs), (1, hs)))], [h_mid, h_other], **e1)
        s_mid = permute('x', s_mid)
        s_full, = run_block(own_len, enc_norm, 1, 'self', [job(True, src, src, flat((0, src)))], [h_full], **e1)
        s_other = permute('y', s_mid)
        z_full, = run_block(own_len, dec_norm, 0, 'self', [job(True, tgt, tgt, y_full, FULL_CHUNKS, part=flat((1, tgt)))],
                        [y_dec, pd_full], pieces=w[4], part_in=True)

        def cross_mid(z, layer, **kwargs):
            return run_block((pair_len, pair_len), dec_norm, layer, 'cross', [job(False, ht, src, flat((0, ht)), src=flat((1, hs), (2, hs)))],
                         [z, s_mid, s_other], own=c_own, gain=1, ff_gain=2, **kwargs)[0]

        def cross_full(z, layer, **kwargs):
            return run_block((pair_len, pair_len), dec_norm, layer, 'cross', [job(True, tgt, src, flat((0, tgt)), src=flat((1, src)))],
                         [z, s_full], own=c_own, gain=1, ff_gain=2, **kwargs)[0]

        cross0 = dict(pieces=w[5], ff=(dec_w1, dec_w2, w[6], w[6]), down_base=D)
        cross1 = dict(pieces=w[7], base=D, ff=(dec_w1, dec_w2, w[8], w[8]), down_base=D)
        z_mid = cross_mid(z_mid, 0, **cross0)
        z_other = permute('y', z_mid)
        z_full = cross_full(z_full, 0, **cross0)
        z_full, = run_block(own_len, dec_norm, 1, 'self', [job(True, tgt, tgt, flat((0, tgt)), FULL_CHUNKS)], [z_full], own=d_own, pieces=w[7])
        z_full = cross_full(z_full, 1, **cross1)
        z_full_other = permute('y', z_full)
        z_mid, = run_block(own_len, dec_norm, 1, 'self', [job(False, ht, tgt, flat((0, ht), (1, ht)), MID_CHUNKS)], [z_mid, z_other],
                       own=d_own, pieces=w[7])
        z_mid = cross_mid(z_mid, 1, **cross1)
        z_mid_other = permute('y', z_mid)

        first = lax.axis_index('model') == 0
        a, b, oa, ob = z_mid[:CHUNK], z_mid[CHUNK:], z_mid_other[:CHUNK], z_mid_other[CHUNK:]
        row_mid = jnp.where(first, jnp.concatenate([a, oa, ob, b], axis=0), jnp.concatenate([oa, a, b, ob], axis=0))
        return jnp.stack([jnp.where(first, z_full, z_full_other), row_mid, jnp.where(first, z_full_other, z_full)])

    return jax.shard_map(local_step, mesh=mesh, in_specs=in_specs_all, out_specs=row_spec, check_vma=False)
```

```python
import functools
import math

import jax
import jax.numpy as jnp
from jax import lax
from jax.experimental import pallas as pl
from jax.experimental.pallas import tpu as pltpu
from jax.sharding import PartitionSpec as P


D = 768
HALF = 384
FF = 3072
NORM_EPS = 1e-6
NEG_BIG = -1e30
EXP_SCALE = 0.125 * math.log2(math.e)
GELU_C = math.sqrt(2.0 / math.pi)
PIECE_XOR = (0, 2, 1, 3)
QROWS = 192
OROWS = 96
TILE = 256
CHUNK = 256
LANES = 128
SUB = 16
HEAD_DIM = 64
VMEM_LIMIT = 60 * 1024 * 1024


def norm_rows(h, gain):
    hf = h.astype(jnp.float32)
    inv = lax.rsqrt(jnp.mean(hf * hf, axis=-1, keepdims=True) + NORM_EPS)
    return (hf * inv * gain).astype(jnp.bfloat16)


def gelu(x):
    return x * (0.5 + 0.5 * jnp.tanh(GELU_C * (x + 0.044715 * (x * x * x))))


def dot(a, b):
    return jnp.dot(a, b, preferred_element_type=jnp.float32)


def dot_t(a, b):
    return lax.dot_general(a, b, (((1,), (1,)), ((), ())), preferred_element_type=jnp.float32)


def runs_of(chunks):
    runs = []
    for c in chunks:
        if runs and runs[-1][0] + runs[-1][1] == c:
            runs[-1] = (runs[-1][0], runs[-1][1] + 1)
        else:
            runs.append((c, 1))
    return runs


def row_copies(src, dst, sem, step):
    rows = src.shape[0]
    return [pltpu.make_async_copy(src.at[pl.ds(r, step), :], dst.at[pl.ds(r, step), :], sem) for r in range(0, rows, step)]


def attn_weight_copies(stage, own, pieces, base, halves, w_s, wo_s, sems):
    ncol = HALF * len(halves)
    off = ncol - HALF
    qkv, out = [], []
    if own:
        for c, src in enumerate(own[:-1]):
            qkv += row_copies(src, w_s.at[:, pl.ds(c * ncol, HALF)], sems[0], QROWS)
        out += row_copies(own[-1], wo_s.at[pl.ds(0, HALF), :], sems[1], OROWS)
    for piece, mask in zip(pieces, PIECE_XOR):
        quarter = stage ^ mask
        r0 = pl.multiple_of(quarter * QROWS, QROWS)
        for c in range(3):
            qkv.append(pltpu.make_async_copy(piece.at[pl.ds(base + c * QROWS, QROWS), :],
                                             w_s.at[pl.ds(r0, QROWS), pl.ds(c * ncol + off, HALF)], sems[0]))
        r1 = pl.multiple_of(off + quarter * OROWS, OROWS)
        for c in range(2):
            out.append(pltpu.make_async_copy(piece.at[pl.ds(base + 3 * QROWS + c * OROWS, OROWS), :],
                                             wo_s.at[pl.ds(r1, OROWS), pl.ds(c * HALF, HALF)], sems[1]))
    return qkv, out


def ff_weight_copies(layer, stage, w1_ref, w2_ref, up_pieces, down_pieces, up_base, down_base, w1_s, w2_s, sems):
    hf = FF // 2
    own_up = row_copies(w1_ref.at[layer], w1_s.at[:, pl.ds(0, hf)], sems[0], OROWS // 2)
    own_down = row_copies(w2_ref.at[layer], w2_s.at[pl.ds(0, hf), :], sems[1], OROWS)
    up, down = [], []
    for i, mask in enumerate(PIECE_XOR):
        quarter = stage ^ mask
        r0 = pl.multiple_of(quarter * QROWS, QROWS)
        for c in range(4):
            up.append(pltpu.make_async_copy(up_pieces[i].at[pl.ds(up_base + c * QROWS, QROWS), :],
                                            w1_s.at[pl.ds(r0, QROWS), pl.ds(hf + c * HALF, HALF)], sems[2]))
        r1 = pl.multiple_of(hf + quarter * HALF, HALF)
        for c in range(2):
            down.append(pltpu.make_async_copy(down_pieces[i].at[pl.ds(down_base + c * HALF, HALF), :],
                                              w2_s.at[pl.ds(r1, HALF), pl.ds(c * HALF, HALF)], sems[3]))
    return [own_up, own_down, up, down]


def start_all(copies):
    for copy in copies:
        copy.start()


def wait_all(copies):
    for copy in copies:
        copy.wait()


def ff_rows(h1, gain, w1_s, w2_s, waits=None):
    xn = norm_rows(h1, gain)
    acc = None
    for c in range(FF // D):
        cols = slice(c * D, (c + 1) * D)
        second = c * D >= FF // 2
        if waits is not None and c in (0, FF // D // 2):
            wait_all(waits[2 * second])
        act = gelu(dot(xn, w1_s[:, cols])).astype(jnp.bfloat16)
        if waits is not None and c in (0, FF // D // 2):
            wait_all(waits[2 * second + 1])
        term = dot(act, w2_s[cols, :])
        acc = term if acc is None else acc + term
    return (h1.astype(jnp.float32) + acc).astype(jnp.bfloat16)


def pack_kernel(cfg, *refs):
    nout = len(cfg['groups']) + (cfg['row'] is not None)
    ins, outs, bufs, sems = refs[:cfg['nin']], refs[cfg['nin']:cfg['nin'] + nout], refs[cfg['nin'] + nout:-1], refs[-1]
    stage = lax.axis_index('stage')
    loads = []
    for g, parts in enumerate(cfg['groups']):
        base, copies = 0, []
        for slot, index in parts:
            ref = ins[slot]
            size = ref.shape[-2] // 4
            for c in range(ref.shape[-1] // HALF):
                src = ref.at[index + (pl.ds(pl.multiple_of(stage * size, size), size), pl.ds(c * HALF, HALF))]
                copies.append(pltpu.make_async_copy(src, bufs[g].at[pl.ds(base, size), :], sems.at[g]))
                base += size
        loads.append(copies)
    if cfg['row'] is not None:
        loads.append(row_copies(ins[cfg['row']].at[2 * lax.axis_index('model')], bufs[-1], sems.at[nout - 1], LANES))
    stores = []
    for copies in loads:
        start_all(copies)
    for g, copies in enumerate(loads):
        wait_all(copies)
        stores += row_copies(bufs[g], outs[g], sems.at[nout + g], QROWS)
        start_all(stores[-(bufs[g].shape[0] // QROWS):])
    wait_all(stores)


def group_rows(sources, parts):
    return sum(sources[slot].shape[-2] * sources[slot].shape[-1] // (4 * HALF) for slot, _ in parts)


def run_pack(sources, groups, row=None):
    hbm = pl.BlockSpec(memory_space=pl.ANY)
    shapes = [jax.ShapeDtypeStruct((group_rows(sources, parts), HALF), jnp.bfloat16) for parts in groups]
    if row is not None:
        shapes.append(jax.ShapeDtypeStruct(sources[row].shape[1:], jnp.bfloat16))
    return pl.pallas_call(
        functools.partial(pack_kernel, dict(nin=len(sources), groups=groups, row=row)),
        out_shape=shapes,
        in_specs=[hbm] * len(sources),
        out_specs=[hbm] * len(shapes),
        scratch_shapes=[pltpu.VMEM(shape.shape, shape.dtype) for shape in shapes] + [pltpu.SemaphoreType.DMA((2 * len(shapes),))],
        compiler_params=pltpu.CompilerParams(vmem_limit_bytes=VMEM_LIMIT),
        cost_estimate=pl.CostEstimate(flops=0, bytes_accessed=sum(4 * shape.size for shape in shapes), transcendentals=0),
    )(*sources)


def rows_at(i, size):
    return pl.ds(pl.multiple_of(i * size, size), size)


def project(h_ref, gain, w_s, cols, first, count, tile, dests, npair):
    def body(i, carry):
        rows = rows_at(first // tile + i, tile)
        x = h_ref[rows, :] if gain is None else norm_rows(h_ref[rows, :], gain)
        value = dot(x, w_s[:, cols])
        for d, dst in enumerate(dests):
            for pair in range(npair):
                col = (d * npair + pair) * LANES
                dst[pair, rows, :] = value[:, col:col + LANES].astype(jnp.bfloat16)
        return carry

    lax.fori_loop(0, count // tile, body, 0)


def attention(tq, tk, chunk_plan, pairs, src_len, off_a, off_b, model_idx, q_s, k_s, v_s, km_s, vx_s, ctx_s):
    causal = chunk_plan is not None
    qb = LANES
    npair = pairs
    lane = lax.broadcasted_iota(jnp.int32, (1, LANES), 1)
    lo_f = jnp.where(lane < HEAD_DIM, 1.0, 0.0).astype(jnp.float32)
    masks_f = (lo_f, 1.0 - lo_f)
    masks_b = [mask.astype(jnp.bfloat16) for mask in masks_f]
    nchunk = tk // CHUNK

    def pair_body(pair, carry):
        if not causal:
            k_first = jnp.where(off_a == 0, k_s[pair, 0:SUB, :].astype(jnp.float32)[0:1],
                                k_s[pair, HALF:HALF + SUB, :].astype(jnp.float32)[0:1])
        for c in range(nchunk):
            rows = slice(c * CHUNK, (c + 1) * CHUNK)
            v_f = v_s[pair, rows, :].astype(jnp.float32)
            ones = jnp.ones((CHUNK, LANES), jnp.float32)
            if not causal:
                idx = lax.broadcasted_iota(jnp.int32, (CHUNK, LANES), 0) + c * CHUNK
                pos = jnp.where(idx < HALF, idx + off_a, idx + (off_b - HALF))
                ok = pos < src_len
                km_s[rows, :] = jnp.where(ok, k_s[pair, rows, :].astype(jnp.float32), k_first).astype(jnp.bfloat16)
                v_f = jnp.where(ok, v_f, 0.0)
                ones = jnp.where(ok, ones, 0.0)
            for head, mask in enumerate(masks_f):
                vrows = slice((2 * c + head) * CHUNK, (2 * c + head + 1) * CHUNK)
                vx_s[vrows, :LANES] = (v_f * mask).astype(jnp.bfloat16)
                vx_s[vrows, LANES:] = (ones * mask).astype(jnp.bfloat16)
        for b in range(tq // qb):
            rows = slice(b * qb, (b + 1) * qb)
            qp = q_s[pair, rows, :]
            q2 = jnp.concatenate([qp * mask for mask in masks_b], axis=0)
            chunks, masks = chunk_plan[b * qb // CHUNK] if causal else (list(range(nchunk)), {})
            parts = []
            for start, count in runs_of(chunks):
                krows = slice(start * CHUNK, (start + count) * CHUNK)
                s_run = dot_t(q2, k_s[pair, krows, :] if causal else km_s[krows, :])
                for j in range(count):
                    s_c = s_run[:, j * CHUNK:(j + 1) * CHUNK]
                    kind = masks.get(start + j)
                    if kind == 'diag':
                        q_idx = lax.broadcasted_iota(jnp.int32, (2 * qb, CHUNK), 0)
                        q_idx = jnp.where(q_idx < qb, q_idx, q_idx - qb) + (b * qb % CHUNK)
                        k_idx = lax.broadcasted_iota(jnp.int32, (2 * qb, CHUNK), 1)
                        s_c = jnp.where(k_idx <= q_idx, s_c, NEG_BIG)
                    elif kind is not None:
                        s_c = jnp.where(model_idx == kind, s_c, NEG_BIG)
                    parts.append(s_c)
            top = functools.reduce(jnp.maximum, parts)
            top = jnp.max(top, axis=-1, keepdims=True)
            probs = [jnp.exp2((part - top) * EXP_SCALE).astype(jnp.bfloat16) for part in parts]
            terms = []
            for start, count in runs_of(chunks):
                used, probs = probs[:count], probs[count:]
                lhs = [half for prob in used for half in (prob[:qb], prob[qb:])]
                terms.append(dot(jnp.concatenate(lhs, axis=1), vx_s[2 * start * CHUNK:2 * (start + count) * CHUNK, :]))
            total = functools.reduce(jnp.add, terms)
            ctx_s[pair, rows, :] = (total[:, :LANES] / total[:, LANES:]).astype(jnp.bfloat16)
        return carry

    lax.fori_loop(0, npair, pair_body, 0)


def block_kernel(cfg, *refs):
    it = iter(refs)

    def take(n):
        return [next(it) for _ in range(n)]

    layer, phases, ff, jobs = cfg['layer'], cfg['phases'], cfg['ff'], cfg['jobs']
    njobs, nphase = len(jobs), len(phases)
    lens_mid, lens_full, norm_in = take(3)
    final_in = take(1)[0] if cfg['final'] else None
    data = take(cfg['ndata'])
    phase_refs = [(take(phase['nown']), take(phase['npiece'])) for phase in phases]
    if ff:
        w1_ref, w2_ref = take(2)
        up_pieces, down_pieces = take(4), take(4)
    outs, h_bufs = take(njobs), take(njobs)
    s_bufs = take(njobs) if cfg['has_src'] else None
    p_bufs = take(njobs) if cfg['part_in'] else None
    o_bufs = take(njobs)
    weight_bufs = [take(2) for _ in phases]
    if phases:
        q_s, k_s, v_s, km_s, vx_s, ctx_s = take(6)
    if ff:
        w1_s, w2_s = take(2)
    norm_ref = take(1)[0]
    final_ref = take(1)[0] if cfg['final'] else None
    sem, job_sem, out_sem = take(3)
    m, stage = lax.axis_index('model'), lax.axis_index('stage')

    def load(parts, dst, semaphore):
        copies, base = [], 0
        for slot, lead, size, steps in parts:
            for a, b in steps:
                start = pl.multiple_of((a + b * m) * size, size) if lead is not None else 0
                src = data[slot]
                if lead is not None:
                    src = src.at[lead[0] + lead[1] * m]
                copies += row_copies(src.at[pl.ds(start, size), :], dst.at[pl.ds(base, size), :], semaphore, LANES)
                base += size
        return copies

    job_copies = []
    for j, job in enumerate(jobs):
        copies = load(job['h'], h_bufs[j], job_sem.at[j])
        if cfg['has_src']:
            copies += load(job['src'], s_bufs[j], job_sem.at[j])
        if cfg['part_in']:
            copies += load(job['part'], p_bufs[j], job_sem.at[j])
        job_copies.append(copies)
    job_copies[0].append(pltpu.make_async_copy(norm_in, norm_ref, job_sem.at[0]))
    if final_ref is not None:
        job_copies[0].append(pltpu.make_async_copy(final_in, final_ref, job_sem.at[0]))
    start_all(job_copies[0])
    weights = []
    for p, phase in enumerate(phases):
        own_refs, pieces = phase_refs[p]
        own = []
        if own_refs and phase['cross']:
            own = [own_refs[0].at[layer], own_refs[1].at[layer, 0], own_refs[1].at[layer, 1], own_refs[2].at[layer]]
        elif own_refs:
            own = [own_refs[0].at[layer, c] for c in range(3)] + [own_refs[1].at[layer]]
        weights.append(attn_weight_copies(stage, own, pieces, phase['base'], phase['halves'], *weight_bufs[p],
                                          [sem.at[2 * p], sem.at[2 * p + 1]]))
    if phases:
        start_all(weights[0][0] + weights[0][1])
    for copies in job_copies[1:]:
        start_all(copies)
    later = [copy for qkv, out in weights[1:] for copy in qkv + out]
    ff_groups = []
    if ff:
        ff_groups = ff_weight_copies(layer, stage, w1_ref, w2_ref, up_pieces, down_pieces, cfg['up_base'], cfg['down_base'], w1_s, w2_s,
                                     [sem.at[4 + i] for i in range(4)])
        later += [copy for group in ff_groups for copy in group]
    if not phases:
        start_all(later)

    wait_all(job_copies[0])
    gain_f = norm_ref[layer, cfg['ff_gain']][None, :]
    for j, job in enumerate(jobs):
        tq = job['tq']
        tile = TILE if tq % TILE == 0 else HALF
        h_ref, o_ref, out = h_bufs[j], o_bufs[j], outs[j]
        if j > 0:
            wait_all(job_copies[j])

        def finish(rows, value, o_ref=o_ref, out=out):
            if final_ref is not None:
                value = norm_rows(value, final_ref[...][None, :])
            o_ref[rows, :] = value
            pltpu.make_async_copy(o_ref.at[rows, :], out.at[rows, :], out_sem).start()

        for p, phase in enumerate(phases):
            tk = job['tks'][p]
            npair = 3 * len(phase['halves'])
            ncol = npair * LANES
            w_s, wo_s = weight_bufs[p]
            gain = norm_ref[layer, phase['gain']][None, :]
            if j == 0:
                wait_all(weights[p][0])
                if p == 0:
                    start_all(later)
            if phase['cross']:
                project(h_ref, gain, w_s, slice(0, ncol), 0, tq, tile, [q_s], npair)
                project(s_bufs[j], None, w_s, slice(ncol, 3 * ncol), 0, tk, TILE, [k_s, v_s], npair)
            else:
                project(h_ref, gain, w_s, slice(0, 3 * ncol), 0, tq, tile, [q_s, k_s, v_s], npair)
                if tk > tq:
                    project(h_ref, gain, w_s, slice(ncol, 3 * ncol), tq, tk - tq, tile, [k_s, v_s], npair)
            if job['full']:
                place = (lens_full[2 * m], 0, HALF)
            else:
                place = (lens_mid[1], HALF * m, HALF * (1 - m))
            if phase['cross'] and not job['full']:
                place = (lens_full[1], HALF * m, HALF * (1 - m))
            attention(tq, tk, job['plans'][p], npair, *place, m, q_s, k_s, v_s, km_s, vx_s, ctx_s)
            last = p == nphase - 1
            if j == 0:
                wait_all(weights[p][1])
                if last:
                    for group in ff_groups:
                        wait_all(group)

            def out_tile(i, carry, h_ref=h_ref, o_ref=o_ref, wo_s=wo_s, npair=npair, tile=tile, finish=finish, j=j, p=p, last=last):
                rows = rows_at(i, tile)
                ctx = jnp.concatenate([ctx_s[pair, rows, :] for pair in range(npair)], axis=1)
                update = dot(ctx, wo_s[...])
                if cfg['part_in'] and p == 0:
                    update = update + p_bufs[j][rows, :]
                if cfg['part_out']:
                    finish(rows, update)
                    return carry
                h1 = (h_ref[rows, :].astype(jnp.float32) + update).astype(jnp.bfloat16)
                if not last:
                    o_ref[rows, :] = h1
                    return carry
                finish(rows, ff_rows(h1, gain_f, w1_s, w2_s) if ff else h1)
                return carry

            lax.fori_loop(0, tq // tile, out_tile, 0)
            h_ref = o_ref
        if not phases:
            def ff_tile(i, carry, h_ref=h_ref, tile=tile, finish=finish):
                rows = rows_at(i, tile)
                finish(rows, ff_rows(h_ref[rows, :], gain_f, w1_s, w2_s))
                return carry

            first = 0
            if j == 0:
                finish(pl.ds(0, tile), ff_rows(h_ref[:tile, :], gain_f, w1_s, w2_s, ff_groups))
                first = 1
            if tq // tile > first:
                lax.fori_loop(first, tq // tile, ff_tile, 0)
    for j in range(njobs):
        pltpu.make_async_copy(o_bufs[j], outs[j], out_sem).wait()


FULL_CHUNKS = [(list(range(i + 1)), {i: 'diag'}) for i in range(4)]
MID_CHUNKS = [([0, 2], {0: 'diag', 2: 1}), ([0, 1, 2, 3], {1: 'diag', 3: 0})]


def run_block(lens, norms, layer, phases, jobs, data, *, ff_gain=0, part_in=False, part_out=False, ff=None, up_base=0, down_base=0,
              final_gain=None):
    bf = jnp.bfloat16
    infos, weights = [], []
    for phase in phases:
        own, pieces = phase.get('own', ()), phase.get('pieces', ())
        halves = ((0,) if own else ()) + ((1,) if pieces else ())
        infos.append(dict(cross=phase['cross'], gain=phase['gain'], base=phase.get('base', 0), halves=halves, nown=len(own), npiece=len(pieces)))
        weights += list(own) + list(pieces)
    has_src = any(info['cross'] for info in infos)
    cfg = dict(layer=layer, phases=infos, ff=ff is not None, jobs=jobs, ndata=len(data), up_base=up_base, down_base=down_base, ff_gain=ff_gain,
               part_in=part_in, part_out=part_out, final=final_gain is not None, has_src=has_src)
    hbm = pl.BlockSpec(memory_space=pl.ANY)
    head = [norms] + ([final_gain] if final_gain is not None else [])
    rest = head + list(data) + weights
    if ff is not None:
        rest += [ff[0], ff[1]] + list(ff[2]) + list(ff[3])
    odt = jnp.float32 if part_out else bf
    tq = max(job['tq'] for job in jobs)
    self_first = bool(infos) and not infos[0]['cross']
    scratch = [pltpu.VMEM((job['tks'][0] if self_first else job['tq'], D), bf) for job in jobs]
    if has_src:
        scratch += [pltpu.VMEM((job['tks'][-1], D), bf) for job in jobs]
    if part_in:
        scratch += [pltpu.VMEM((job['tq'], D), jnp.float32) for job in jobs]
    scratch += [pltpu.VMEM((job['tq'], D), odt) for job in jobs]
    for info in infos:
        cols = len(info['halves']) * HALF
        scratch += [pltpu.VMEM((D, 3 * cols), bf), pltpu.VMEM((cols, D), bf)]
    scores = 0
    if infos:
        tk = max(max(job['tks']) for job in jobs)
        npair = max(3 * len(info['halves']) for info in infos)
        scratch += [pltpu.VMEM(shape, bf) for shape in [
            (npair, tq, LANES), (npair, tk, LANES), (npair, tk, LANES), (tk, LANES), (2 * tk, 2 * LANES), (npair, tq, LANES)]]
        scores = sum(job['tq'] * size * npair * 2 for job in jobs for size in job['tks'])
    if ff is not None:
        scratch += [pltpu.VMEM((D, FF), bf), pltpu.VMEM((FF, D), bf)]
    scratch += [pltpu.VMEM(value.shape, jnp.float32) for value in head]
    scratch += [pltpu.SemaphoreType.DMA((8,)), pltpu.SemaphoreType.DMA((2,)), pltpu.SemaphoreType.DMA]
    rows_q = sum(job['tq'] for job in jobs)
    flops = scores * 512 + 8 * D * D * len(infos) * rows_q + (4 * D * FF * rows_q if ff is not None else 0)
    nbytes = 4 * D * rows_q + 8 * D * D * len(infos) + (4 * D * FF if ff is not None else 0)
    return pl.pallas_call(
        functools.partial(block_kernel, cfg),
        out_shape=[jax.ShapeDtypeStruct((job['tq'], D), odt) for job in jobs],
        in_specs=[pl.BlockSpec(memory_space=pltpu.SMEM)] * 2 + [hbm] * len(rest),
        out_specs=[hbm] * len(jobs),
        scratch_shapes=scratch,
        compiler_params=pltpu.CompilerParams(vmem_limit_bytes=VMEM_LIMIT),
        cost_estimate=pl.CostEstimate(flops=flops, bytes_accessed=nbytes, transcendentals=scores),
    )(*lens, *rest)


def solution(mesh):
    row_spec = P(('data', 'stage'), None, None)
    len_spec = P(('data', 'stage'))
    qkv_spec = P(None, None, None, 'model')
    col_spec = P(None, None, 'model')
    row_w_spec = P(None, 'model', None)
    rep_spec = P()
    in_specs_all = (row_spec, len_spec, row_spec, qkv_spec, row_w_spec, col_spec, row_w_spec, rep_spec, rep_spec,
                    qkv_spec, row_w_spec, col_spec, qkv_spec, row_w_spec, col_spec, row_w_spec, rep_spec)
    perms = dict(y=('model', [(0, 1), (1, 0)]), x=('stage', [(i, i ^ 2) for i in range(4)]), c=('stage', [(i, i ^ 1) for i in range(4)]))

    def permute(kind, value):
        return lax.ppermute(value, *perms[kind])

    def spread(pack):
        first = permute('y', pack)
        second = permute('x', first)
        return [first, second, permute('c', first), permute('c', second)]

    def local_step(x_enc, enc_len, y_dec, enc_wqkv, enc_wo, enc_w1, enc_w2, enc_norm, enc_final,
                   dec_wqkv, dec_wo, crs_wq, crs_wkv, crs_wo, dec_w1, dec_w2, dec_norm):
        src, tgt = x_enc.shape[1], y_dec.shape[1]
        enc_qkv_t, dec_qkv_t, crs_kv_t = [jnp.transpose(w, (0, 2, 1, 3)) for w in (enc_wqkv, dec_wqkv, crs_wkv)]
        pair_len = permute('x', enc_len)
        own_len = (enc_len, pair_len)

        sources_a = [enc_qkv_t, enc_wo, enc_w1, enc_w2, dec_qkv_t, dec_wo]
        sources_b = sources_a + [crs_wq, crs_kv_t, crs_wo, dec_w1, dec_w2]

        def self_parts(slot, layer):
            return [(slot, (layer, c)) for c in range(3)] + [(slot + 1, (layer,))]

        def cross_parts(layer):
            return [(6, (layer,))] + [(7, (layer, c)) for c in range(2)] + [(8, (layer,))]

        def one(slot, layer):
            return [(slot, (layer,))]

        groups_a = [self_parts(0, 0), one(2, 0) + one(3, 0)]
        groups_b = [self_parts(0, 1), one(2, 1) + one(3, 1), self_parts(4, 0), cross_parts(0) + one(9, 0) + one(10, 0),
                    self_parts(4, 1) + cross_parts(1), one(9, 1) + one(10, 1)]
        *packs, x_row = run_pack(sources_a[:4] + [x_enc], groups_a, row=4)
        packs += list(run_pack(sources_b, groups_b))
        x_row = permute('x', x_row)
        w = [spread(pack) for pack in packs]

        full_lead, mid_lead = (0, 2), (1, 0)
        same = [(0, 0)]

        def job(full, tq, tks, h, plans=(None,), **extra):
            return dict(full=full, tq=tq, tks=tks, h=h, plans=plans, **extra)

        def flat(*slots_sizes):
            return [(slot, None, size, same) for slot, size in slots_sizes]

        hs, ht = src // 2, tgt // 2
        x_mid = [(0, mid_lead, hs, [(0, 1), (1, -1)])]
        y_mid = [(0, mid_lead, CHUNK, [(0, 1), (3, -1), (1, -1), (2, 1)])]
        y_full = [(0, full_lead, tgt, same)]
        e_own, d_own, c_own = (enc_qkv_t, enc_wo), (dec_qkv_t, dec_wo), (crs_wq, crs_kv_t, crs_wo)

        def self_phase(**kwargs):
            return dict(cross=False, gain=0, **kwargs)

        def cross_phase(**kwargs):
            return dict(cross=True, gain=1, own=c_own, **kwargs)

        mid_plan, full_plan = (MID_CHUNKS, None), (FULL_CHUNKS, None)
        pd_mid, pd_full = run_block(own_len, dec_norm, 0, [self_phase(own=d_own)],
                                [job(False, ht, (tgt,), y_mid, mid_plan), job(True, tgt, (tgt,), y_full, full_plan)], [y_dec], part_out=True)
        pe_mid, pe_full = run_block(own_len, enc_norm, 0, [self_phase(own=e_own)],
                                [job(False, hs, (src,), x_mid), job(True, src, (src,), flat((1, src)))], [x_enc, x_row], part_out=True)
        h_mid, h_full = run_block(own_len, enc_norm, 0, [self_phase(pieces=w[0])],
                              [job(False, hs, (src,), x_mid, part=flat((2, hs))), job(True, src, (src,), flat((1, src)), part=flat((3, src)))],
                              [x_enc, x_row, pe_mid, pe_full], part_in=True)
        h_mid, h_full = run_block(own_len, enc_norm, 0, [], [job(False, hs, (), flat((0, hs))), job(True, src, (), flat((1, src)))],
                              [h_mid, h_full], ff_gain=1, ff=(enc_w1, enc_w2, w[1], w[1]), down_base=D)
        h_other = permute('y', h_mid)
        e1 = dict(ff_gain=1, ff=(enc_w1, enc_w2, w[3], w[3]), down_base=D, final_gain=enc_final)
        e1_phases = [self_phase(own=e_own, pieces=w[2])]
        s_full, = run_block(own_len, enc_norm, 1, e1_phases, [job(True, src, (src,), flat((0, src)))], [h_full], **e1)
        s_mid, = run_block(own_len, enc_norm, 1, e1_phases, [job(False, hs, (src,), flat((0, hs), (1, hs)))], [h_mid, h_other], **e1)
        s_mid = permute('x', s_mid)
        s_other = permute('y', s_mid)

        z_mid, = run_block(own_len, dec_norm, 0, [self_phase(pieces=w[4])],
                       [job(False, ht, (tgt,), y_mid, mid_plan, part=flat((1, ht)))], [y_dec, pd_mid], part_in=True)
        cross0, cross1 = cross_phase(pieces=w[5]), cross_phase(pieces=w[6], base=D)
        ff0 = dict(ff_gain=2, ff=(dec_w1, dec_w2, w[5], w[5]), up_base=D, down_base=2 * D)
        ff1 = dict(ff_gain=2, ff=(dec_w1, dec_w2, w[7], w[7]), down_base=D)
        z_full, = run_block(own_len, dec_norm, 0, [self_phase(pieces=w[4]), cross0],
                        [job(True, tgt, (tgt, src), y_full, full_plan, part=flat((1, tgt)), src=flat((2, src)))], [y_dec, pd_full, s_full],
                        part_in=True, **ff0)
        z_mid, = run_block(own_len, dec_norm, 0, [cross0], [job(False, ht, (src,), flat((0, ht)), src=flat((1, hs), (2, hs)))],
                       [z_mid, s_mid, s_other], **ff0)
        z_other = permute('y', z_mid)
        d1_phases = [self_phase(own=d_own, pieces=w[6]), cross1]
        z_full, = run_block(own_len, dec_norm, 1, d1_phases, [job(True, tgt, (tgt, src), flat((0, tgt)), full_plan, src=flat((1, src)))],
                        [z_full, s_full], **ff1)
        z_full_other = permute('y', z_full)
        z_mid, = run_block(own_len, dec_norm, 1, d1_phases,
                       [job(False, ht, (tgt, src), flat((0, ht), (1, ht)), mid_plan, src=flat((2, hs), (3, hs)))],
                       [z_mid, z_other, s_mid, s_other], **ff1)
        z_mid_other = permute('y', z_mid)

        first = lax.axis_index('model') == 0
        a, b, oa, ob = z_mid[:CHUNK], z_mid[CHUNK:], z_mid_other[:CHUNK], z_mid_other[CHUNK:]
        row_mid = jnp.where(first, jnp.concatenate([a, oa, ob, b], axis=0), jnp.concatenate([oa, a, b, ob], axis=0))
        return jnp.stack([jnp.where(first, z_full, z_full_other), row_mid, jnp.where(first, z_full_other, z_full)])

    return jax.shard_map(local_step, mesh=mesh, in_specs=in_specs_all, out_specs=row_spec, check_vma=False)
```

```python
import functools
import math

import jax
import jax.numpy as jnp
from jax import lax
from jax.experimental import pallas as pl
from jax.experimental.pallas import tpu as pltpu
from jax.sharding import PartitionSpec as P


D = 768
HALF = 384
FF = 3072
NORM_EPS = 1e-6
NEG_BIG = -1e30
EXP_SCALE = 0.125 * math.log2(math.e)
GELU_C = math.sqrt(2.0 / math.pi)
PIECE_XOR = (0, 2, 1, 3)
QROWS = 192
OROWS = 96
TILE = 256
CHUNK = 256
LANES = 128
SUB = 16
HEAD_DIM = 64
VMEM_LIMIT = 60 * 1024 * 1024


def norm_rows(h, gain):
    hf = h.astype(jnp.float32)
    inv = lax.rsqrt(jnp.mean(hf * hf, axis=-1, keepdims=True) + NORM_EPS)
    return (hf * inv * gain).astype(jnp.bfloat16)


def gelu(x):
    return x * (0.5 + 0.5 * jnp.tanh(GELU_C * (x + 0.044715 * (x * x * x))))


def dot(a, b):
    return jnp.dot(a, b, preferred_element_type=jnp.float32)


def dot_t(a, b):
    return lax.dot_general(a, b, (((1,), (1,)), ((), ())), preferred_element_type=jnp.float32)


def runs_of(chunks):
    runs = []
    for c in chunks:
        if runs and runs[-1][0] + runs[-1][1] == c:
            runs[-1] = (runs[-1][0], runs[-1][1] + 1)
        else:
            runs.append((c, 1))
    return runs


def row_copies(src, dst, sem, step):
    rows = src.shape[0]
    return [pltpu.make_async_copy(src.at[pl.ds(r, step), :], dst.at[pl.ds(r, step), :], sem) for r in range(0, rows, step)]


def attn_weight_copies(stage, own, pieces, base, halves, w_s, wo_s, sems):
    ncol = HALF * len(halves)
    off = ncol - HALF
    qkv, out = [], []
    if own:
        for c, src in enumerate(own[:-1]):
            qkv += row_copies(src, w_s.at[:, pl.ds(c * ncol, HALF)], sems[0], QROWS)
        out += row_copies(own[-1], wo_s.at[pl.ds(0, HALF), :], sems[1], OROWS)
    for piece, mask in zip(pieces, PIECE_XOR):
        quarter = stage ^ mask
        r0 = pl.multiple_of(quarter * QROWS, QROWS)
        for c in range(3):
            qkv.append(pltpu.make_async_copy(piece.at[pl.ds(base + c * QROWS, QROWS), :],
                                             w_s.at[pl.ds(r0, QROWS), pl.ds(c * ncol + off, HALF)], sems[0]))
        r1 = pl.multiple_of(off + quarter * OROWS, OROWS)
        for c in range(2):
            out.append(pltpu.make_async_copy(piece.at[pl.ds(base + 3 * QROWS + c * OROWS, OROWS), :],
                                             wo_s.at[pl.ds(r1, OROWS), pl.ds(c * HALF, HALF)], sems[1]))
    return qkv, out


def ff_weight_copies(layer, stage, w1_ref, w2_ref, up_pieces, down_pieces, up_base, down_base, w1_s, w2_s, sems):
    hf = FF // 2
    own_up = row_copies(w1_ref.at[layer], w1_s.at[:, pl.ds(0, hf)], sems[0], OROWS // 2)
    own_down = row_copies(w2_ref.at[layer], w2_s.at[pl.ds(0, hf), :], sems[1], OROWS)
    up, down = [], []
    for i, mask in enumerate(PIECE_XOR):
        quarter = stage ^ mask
        r0 = pl.multiple_of(quarter * QROWS, QROWS)
        for c in range(4):
            up.append(pltpu.make_async_copy(up_pieces[i].at[pl.ds(up_base + c * QROWS, QROWS), :],
                                            w1_s.at[pl.ds(r0, QROWS), pl.ds(hf + c * HALF, HALF)], sems[2]))
        r1 = pl.multiple_of(hf + quarter * HALF, HALF)
        for c in range(2):
            down.append(pltpu.make_async_copy(down_pieces[i].at[pl.ds(down_base + c * HALF, HALF), :],
                                              w2_s.at[pl.ds(r1, HALF), pl.ds(c * HALF, HALF)], sems[3]))
    return [own_up, own_down, up, down]


def start_all(copies):
    for copy in copies:
        copy.start()


def wait_all(copies):
    for copy in copies:
        copy.wait()


def ff_rows(h1, gain, w1_s, w2_s, waits=None):
    xn = norm_rows(h1, gain)
    acc = None
    for c in range(FF // D):
        cols = slice(c * D, (c + 1) * D)
        second = c * D >= FF // 2
        if waits is not None and c in (0, FF // D // 2):
            wait_all(waits[2 * second])
        act = gelu(dot(xn, w1_s[:, cols])).astype(jnp.bfloat16)
        if waits is not None and c in (0, FF // D // 2):
            wait_all(waits[2 * second + 1])
        term = dot(act, w2_s[cols, :])
        acc = term if acc is None else acc + term
    return (h1.astype(jnp.float32) + acc).astype(jnp.bfloat16)


def pack_kernel(cfg, *refs):
    nout = len(cfg['groups']) + (cfg['row'] is not None)
    ins, outs, bufs, sems = refs[:cfg['nin']], refs[cfg['nin']:cfg['nin'] + nout], refs[cfg['nin'] + nout:-1], refs[-1]
    stage = lax.axis_index('stage')
    loads = []
    for g, parts in enumerate(cfg['groups']):
        base, copies = 0, []
        for slot, index in parts:
            ref = ins[slot]
            size = ref.shape[-2] // 4
            for c in range(ref.shape[-1] // HALF):
                src = ref.at[index + (pl.ds(pl.multiple_of(stage * size, size), size), pl.ds(c * HALF, HALF))]
                copies.append(pltpu.make_async_copy(src, bufs[g].at[pl.ds(base, size), :], sems.at[g]))
                base += size
        loads.append(copies)
    if cfg['row'] is not None:
        loads.append(row_copies(ins[cfg['row']].at[2 * lax.axis_index('model')], bufs[-1], sems.at[nout - 1], LANES))
    stores = []
    for copies in loads:
        start_all(copies)
    for g, copies in enumerate(loads):
        wait_all(copies)
        stores += row_copies(bufs[g], outs[g], sems.at[nout + g], QROWS)
        start_all(stores[-(bufs[g].shape[0] // QROWS):])
    wait_all(stores)


def group_rows(sources, parts):
    return sum(sources[slot].shape[-2] * sources[slot].shape[-1] // (4 * HALF) for slot, _ in parts)


def run_pack(sources, groups, row=None):
    hbm = pl.BlockSpec(memory_space=pl.ANY)
    shapes = [jax.ShapeDtypeStruct((group_rows(sources, parts), HALF), jnp.bfloat16) for parts in groups]
    if row is not None:
        shapes.append(jax.ShapeDtypeStruct(sources[row].shape[1:], jnp.bfloat16))
    return pl.pallas_call(
        functools.partial(pack_kernel, dict(nin=len(sources), groups=groups, row=row)),
        out_shape=shapes,
        in_specs=[hbm] * len(sources),
        out_specs=[hbm] * len(shapes),
        scratch_shapes=[pltpu.VMEM(shape.shape, shape.dtype) for shape in shapes] + [pltpu.SemaphoreType.DMA((2 * len(shapes),))],
        compiler_params=pltpu.CompilerParams(vmem_limit_bytes=VMEM_LIMIT),
        cost_estimate=pl.CostEstimate(flops=0, bytes_accessed=sum(4 * shape.size for shape in shapes), transcendentals=0),
    )(*sources)


def rows_at(i, size):
    return pl.ds(pl.multiple_of(i * size, size), size)


def project(h_ref, gain, w_s, cols, first, count, tile, dests, npair):
    def body(i, carry):
        rows = rows_at(first // tile + i, tile)
        x = h_ref[rows, :] if gain is None else norm_rows(h_ref[rows, :], gain)
        value = dot(x, w_s[:, cols])
        for d, dst in enumerate(dests):
            for pair in range(npair):
                col = (d * npair + pair) * LANES
                dst[pair, rows, :] = value[:, col:col + LANES].astype(jnp.bfloat16)
        return carry

    lax.fori_loop(0, count // tile, body, 0)


def attention(tq, tk, chunk_plan, pairs, src_len, off_a, off_b, model_idx, q_s, k_s, v_s, km_s, vx_s, ctx_s):
    causal = chunk_plan is not None
    qb = LANES
    npair = pairs
    lane = lax.broadcasted_iota(jnp.int32, (1, LANES), 1)
    lo_f = jnp.where(lane < HEAD_DIM, 1.0, 0.0).astype(jnp.float32)
    masks_f = (lo_f, 1.0 - lo_f)
    masks_b = [mask.astype(jnp.bfloat16) for mask in masks_f]
    nchunk = tk // CHUNK

    def pair_body(pair, carry):
        if not causal:
            k_first = jnp.where(off_a == 0, k_s[pair, 0:SUB, :].astype(jnp.float32)[0:1],
                                k_s[pair, HALF:HALF + SUB, :].astype(jnp.float32)[0:1])
        for c in range(nchunk):
            rows = slice(c * CHUNK, (c + 1) * CHUNK)
            v_f = v_s[pair, rows, :].astype(jnp.float32)
            ones = jnp.ones((CHUNK, LANES), jnp.float32)
            if not causal:
                idx = lax.broadcasted_iota(jnp.int32, (CHUNK, LANES), 0) + c * CHUNK
                pos = jnp.where(idx < HALF, idx + off_a, idx + (off_b - HALF))
                ok = pos < src_len
                km_s[rows, :] = jnp.where(ok, k_s[pair, rows, :].astype(jnp.float32), k_first).astype(jnp.bfloat16)
                v_f = jnp.where(ok, v_f, 0.0)
                ones = jnp.where(ok, ones, 0.0)
            for head, mask in enumerate(masks_f):
                vrows = slice((2 * c + head) * CHUNK, (2 * c + head + 1) * CHUNK)
                vx_s[vrows, :LANES] = (v_f * mask).astype(jnp.bfloat16)
                vx_s[vrows, LANES:] = (ones * mask).astype(jnp.bfloat16)
        for b in range(tq // qb):
            rows = slice(b * qb, (b + 1) * qb)
            qp = q_s[pair, rows, :]
            q2 = jnp.concatenate([qp * mask for mask in masks_b], axis=0)
            chunks, masks = chunk_plan[b * qb // CHUNK] if causal else (list(range(nchunk)), {})
            parts = []
            for start, count in runs_of(chunks):
                krows = slice(start * CHUNK, (start + count) * CHUNK)
                s_run = dot_t(q2, k_s[pair, krows, :] if causal else km_s[krows, :])
                for j in range(count):
                    s_c = s_run[:, j * CHUNK:(j + 1) * CHUNK]
                    kind = masks.get(start + j)
                    if kind == 'diag':
                        q_idx = lax.broadcasted_iota(jnp.int32, (2 * qb, CHUNK), 0)
                        q_idx = jnp.where(q_idx < qb, q_idx, q_idx - qb) + (b * qb % CHUNK)
                        k_idx = lax.broadcasted_iota(jnp.int32, (2 * qb, CHUNK), 1)
                        s_c = jnp.where(k_idx <= q_idx, s_c, NEG_BIG)
                    elif kind is not None:
                        s_c = jnp.where(model_idx == kind, s_c, NEG_BIG)
                    parts.append(s_c)
            top = functools.reduce(jnp.maximum, parts)
            top = jnp.max(top, axis=-1, keepdims=True)
            probs = [jnp.exp2((part - top) * EXP_SCALE).astype(jnp.bfloat16) for part in parts]
            terms = []
            for start, count in runs_of(chunks):
                used, probs = probs[:count], probs[count:]
                lhs = [half for prob in used for half in (prob[:qb], prob[qb:])]
                terms.append(dot(jnp.concatenate(lhs, axis=1), vx_s[2 * start * CHUNK:2 * (start + count) * CHUNK, :]))
            total = functools.reduce(jnp.add, terms)
            ctx_s[pair, rows, :] = (total[:, :LANES] / total[:, LANES:]).astype(jnp.bfloat16)
        return carry

    lax.fori_loop(0, npair, pair_body, 0, unroll=2 if npair % 2 == 0 else npair)


def block_kernel(cfg, *refs):
    it = iter(refs)

    def take(n):
        return [next(it) for _ in range(n)]

    layer, phases, ff, jobs = cfg['layer'], cfg['phases'], cfg['ff'], cfg['jobs']
    njobs, nphase = len(jobs), len(phases)
    lens_mid, lens_full, norm_in = take(3)
    final_in = take(1)[0] if cfg['final'] else None
    data = take(cfg['ndata'])
    phase_refs = [(take(phase['nown']), take(phase['npiece'])) for phase in phases]
    if ff:
        w1_ref, w2_ref = take(2)
        up_pieces, down_pieces = take(4), take(4)
    outs, h_bufs = take(njobs), take(njobs)
    s_bufs = take(njobs) if cfg['has_src'] else None
    p_bufs = take(njobs) if cfg['part_in'] else None
    o_bufs = take(njobs)
    weight_bufs = [take(2) for _ in phases]
    if phases:
        q_s, k_s, v_s, km_s, vx_s, ctx_s = take(6)
    if ff:
        w1_s, w2_s = take(2)
    norm_ref = take(1)[0]
    final_ref = take(1)[0] if cfg['final'] else None
    sem, job_sem, out_sem = take(3)
    m, stage = lax.axis_index('model'), lax.axis_index('stage')

    def load(parts, dst, semaphore):
        copies, base = [], 0
        for slot, lead, size, steps in parts:
            for a, b in steps:
                start = pl.multiple_of((a + b * m) * size, size) if lead is not None else 0
                src = data[slot]
                if lead is not None:
                    src = src.at[lead[0] + lead[1] * m]
                copies += row_copies(src.at[pl.ds(start, size), :], dst.at[pl.ds(base, size), :], semaphore, LANES)
                base += size
        return copies

    job_copies = []
    for j, job in enumerate(jobs):
        copies = load(job['h'], h_bufs[j], job_sem.at[j])
        if cfg['has_src']:
            copies += load(job['src'], s_bufs[j], job_sem.at[j])
        if cfg['part_in']:
            copies += load(job['part'], p_bufs[j], job_sem.at[j])
        job_copies.append(copies)
    job_copies[0].append(pltpu.make_async_copy(norm_in, norm_ref, job_sem.at[0]))
    if final_ref is not None:
        job_copies[0].append(pltpu.make_async_copy(final_in, final_ref, job_sem.at[0]))
    start_all(job_copies[0])
    weights = []
    for p, phase in enumerate(phases):
        own_refs, pieces = phase_refs[p]
        own = []
        if own_refs and phase['cross']:
            own = [own_refs[0].at[layer], own_refs[1].at[layer, 0], own_refs[1].at[layer, 1], own_refs[2].at[layer]]
        elif own_refs:
            own = [own_refs[0].at[layer, c] for c in range(3)] + [own_refs[1].at[layer]]
        weights.append(attn_weight_copies(stage, own, pieces, phase['base'], phase['halves'], *weight_bufs[p],
                                          [sem.at[2 * p], sem.at[2 * p + 1]]))
    if phases:
        start_all(weights[0][0] + weights[0][1])
    for copies in job_copies[1:]:
        start_all(copies)
    later = [copy for qkv, out in weights[1:] for copy in qkv + out]
    ff_groups = []
    if ff:
        ff_groups = ff_weight_copies(layer, stage, w1_ref, w2_ref, up_pieces, down_pieces, cfg['up_base'], cfg['down_base'], w1_s, w2_s,
                                     [sem.at[4 + i] for i in range(4)])
        later += [copy for group in ff_groups for copy in group]
    if not phases:
        start_all(later)

    wait_all(job_copies[0])
    gain_f = norm_ref[layer, cfg['ff_gain']][None, :]
    for j, job in enumerate(jobs):
        tq = job['tq']
        tile = TILE if tq % TILE == 0 else HALF
        h_ref, o_ref, out = h_bufs[j], o_bufs[j], outs[j]
        if j > 0:
            wait_all(job_copies[j])

        def finish(rows, value, o_ref=o_ref, out=out):
            if final_ref is not None:
                value = norm_rows(value, final_ref[...][None, :])
            o_ref[rows, :] = value
            pltpu.make_async_copy(o_ref.at[rows, :], out.at[rows, :], out_sem).start()

        for p, phase in enumerate(phases):
            tk = job['tks'][p]
            npair = 3 * len(phase['halves'])
            ncol = npair * LANES
            w_s, wo_s = weight_bufs[p]
            gain = norm_ref[layer, phase['gain']][None, :]
            if j == 0:
                wait_all(weights[p][0])
                if p == 0:
                    start_all(later)
            if phase['cross']:
                project(h_ref, gain, w_s, slice(0, ncol), 0, tq, tile, [q_s], npair)
                project(s_bufs[j], None, w_s, slice(ncol, 3 * ncol), 0, tk, TILE, [k_s, v_s], npair)
            else:
                project(h_ref, gain, w_s, slice(0, 3 * ncol), 0, tq, tile, [q_s, k_s, v_s], npair)
                if tk > tq:
                    project(h_ref, gain, w_s, slice(ncol, 3 * ncol), tq, tk - tq, tile, [k_s, v_s], npair)
            if job['full']:
                place = (lens_full[2 * m], 0, HALF)
            else:
                place = (lens_mid[1], HALF * m, HALF * (1 - m))
            if phase['cross'] and not job['full']:
                place = (lens_full[1], HALF * m, HALF * (1 - m))
            attention(tq, tk, job['plans'][p], npair, *place, m, q_s, k_s, v_s, km_s, vx_s, ctx_s)
            last = p == nphase - 1
            if j == 0:
                wait_all(weights[p][1])
                if last:
                    for group in ff_groups:
                        wait_all(group)

            def out_tile(i, carry, h_ref=h_ref, o_ref=o_ref, wo_s=wo_s, npair=npair, tile=tile, finish=finish, j=j, p=p, last=last):
                rows = rows_at(i, tile)
                ctx = jnp.concatenate([ctx_s[pair, rows, :] for pair in range(npair)], axis=1)
                update = dot(ctx, wo_s[...])
                if cfg['part_in'] and p == 0:
                    update = update + p_bufs[j][rows, :]
                if cfg['part_out']:
                    finish(rows, update)
                    return carry
                h1 = (h_ref[rows, :].astype(jnp.float32) + update).astype(jnp.bfloat16)
                if not last:
                    o_ref[rows, :] = h1
                    return carry
                finish(rows, ff_rows(h1, gain_f, w1_s, w2_s) if ff else h1)
                return carry

            lax.fori_loop(0, tq // tile, out_tile, 0)
            h_ref = o_ref
        if not phases:
            def ff_tile(i, carry, h_ref=h_ref, tile=tile, finish=finish):
                rows = rows_at(i, tile)
                finish(rows, ff_rows(h_ref[rows, :], gain_f, w1_s, w2_s))
                return carry

            first = 0
            if j == 0:
                finish(pl.ds(0, tile), ff_rows(h_ref[:tile, :], gain_f, w1_s, w2_s, ff_groups))
                first = 1
            if tq // tile > first:
                lax.fori_loop(first, tq // tile, ff_tile, 0)
    for j in range(njobs):
        pltpu.make_async_copy(o_bufs[j], outs[j], out_sem).wait()


FULL_CHUNKS = [(list(range(i + 1)), {i: 'diag'}) for i in range(4)]
MID_CHUNKS = [([0, 2], {0: 'diag', 2: 1}), ([0, 1, 2, 3], {1: 'diag', 3: 0})]


def run_block(lens, norms, layer, phases, jobs, data, *, ff_gain=0, part_in=False, part_out=False, ff=None, up_base=0, down_base=0,
              final_gain=None):
    bf = jnp.bfloat16
    infos, weights = [], []
    for phase in phases:
        own, pieces = phase.get('own', ()), phase.get('pieces', ())
        halves = ((0,) if own else ()) + ((1,) if pieces else ())
        infos.append(dict(cross=phase['cross'], gain=phase['gain'], base=phase.get('base', 0), halves=halves, nown=len(own), npiece=len(pieces)))
        weights += list(own) + list(pieces)
    has_src = any(info['cross'] for info in infos)
    cfg = dict(layer=layer, phases=infos, ff=ff is not None, jobs=jobs, ndata=len(data), up_base=up_base, down_base=down_base, ff_gain=ff_gain,
               part_in=part_in, part_out=part_out, final=final_gain is not None, has_src=has_src)
    hbm = pl.BlockSpec(memory_space=pl.ANY)
    head = [norms] + ([final_gain] if final_gain is not None else [])
    rest = head + list(data) + weights
    if ff is not None:
        rest += [ff[0], ff[1]] + list(ff[2]) + list(ff[3])
    odt = jnp.float32 if part_out else bf
    tq = max(job['tq'] for job in jobs)
    self_first = bool(infos) and not infos[0]['cross']
    scratch = [pltpu.VMEM((job['tks'][0] if self_first else job['tq'], D), bf) for job in jobs]
    if has_src:
        scratch += [pltpu.VMEM((job['tks'][-1], D), bf) for job in jobs]
    if part_in:
        scratch += [pltpu.VMEM((job['tq'], D), jnp.float32) for job in jobs]
    scratch += [pltpu.VMEM((job['tq'], D), odt) for job in jobs]
    for info in infos:
        cols = len(info['halves']) * HALF
        scratch += [pltpu.VMEM((D, 3 * cols), bf), pltpu.VMEM((cols, D), bf)]
    scores = 0
    if infos:
        tk = max(max(job['tks']) for job in jobs)
        npair = max(3 * len(info['halves']) for info in infos)
        scratch += [pltpu.VMEM(shape, bf) for shape in [
            (npair, tq, LANES), (npair, tk, LANES), (npair, tk, LANES), (tk, LANES), (2 * tk, 2 * LANES), (npair, tq, LANES)]]
        scores = sum(job['tq'] * size * npair * 2 for job in jobs for size in job['tks'])
    if ff is not None:
        scratch += [pltpu.VMEM((D, FF), bf), pltpu.VMEM((FF, D), bf)]
    scratch += [pltpu.VMEM(value.shape, jnp.float32) for value in head]
    scratch += [pltpu.SemaphoreType.DMA((8,)), pltpu.SemaphoreType.DMA((2,)), pltpu.SemaphoreType.DMA]
    rows_q = sum(job['tq'] for job in jobs)
    flops = scores * 512 + 8 * D * D * len(infos) * rows_q + (4 * D * FF * rows_q if ff is not None else 0)
    nbytes = 4 * D * rows_q + 8 * D * D * len(infos) + (4 * D * FF if ff is not None else 0)
    return pl.pallas_call(
        functools.partial(block_kernel, cfg),
        out_shape=[jax.ShapeDtypeStruct((job['tq'], D), odt) for job in jobs],
        in_specs=[pl.BlockSpec(memory_space=pltpu.SMEM)] * 2 + [hbm] * len(rest),
        out_specs=[hbm] * len(jobs),
        scratch_shapes=scratch,
        compiler_params=pltpu.CompilerParams(vmem_limit_bytes=VMEM_LIMIT),
        cost_estimate=pl.CostEstimate(flops=flops, bytes_accessed=nbytes, transcendentals=scores),
    )(*lens, *rest)


def solution(mesh):
    row_spec = P(('data', 'stage'), None, None)
    len_spec = P(('data', 'stage'))
    qkv_spec = P(None, None, None, 'model')
    col_spec = P(None, None, 'model')
    row_w_spec = P(None, 'model', None)
    rep_spec = P()
    in_specs_all = (row_spec, len_spec, row_spec, qkv_spec, row_w_spec, col_spec, row_w_spec, rep_spec, rep_spec,
                    qkv_spec, row_w_spec, col_spec, qkv_spec, row_w_spec, col_spec, row_w_spec, rep_spec)
    perms = dict(y=('model', [(0, 1), (1, 0)]), x=('stage', [(i, i ^ 2) for i in range(4)]), c=('stage', [(i, i ^ 1) for i in range(4)]))

    def permute(kind, value):
        return lax.ppermute(value, *perms[kind])

    def spread(pack):
        first = permute('y', pack)
        second = permute('x', first)
        return [first, second, permute('c', first), permute('c', second)]

    def local_step(x_enc, enc_len, y_dec, enc_wqkv, enc_wo, enc_w1, enc_w2, enc_norm, enc_final,
                   dec_wqkv, dec_wo, crs_wq, crs_wkv, crs_wo, dec_w1, dec_w2, dec_norm):
        src, tgt = x_enc.shape[1], y_dec.shape[1]
        enc_qkv_t, dec_qkv_t, crs_kv_t = [jnp.transpose(w, (0, 2, 1, 3)) for w in (enc_wqkv, dec_wqkv, crs_wkv)]
        pair_len = permute('x', enc_len)
        own_len = (enc_len, pair_len)

        sources_a = [enc_qkv_t, enc_wo, enc_w1, enc_w2, dec_qkv_t, dec_wo]
        sources_b = sources_a + [crs_wq, crs_kv_t, crs_wo, dec_w1, dec_w2]

        def self_parts(slot, layer):
            return [(slot, (layer, c)) for c in range(3)] + [(slot + 1, (layer,))]

        def cross_parts(layer):
            return [(6, (layer,))] + [(7, (layer, c)) for c in range(2)] + [(8, (layer,))]

        def one(slot, layer):
            return [(slot, (layer,))]

        groups_a = [self_parts(0, 0), one(2, 0) + one(3, 0)]
        groups_b = [self_parts(0, 1), one(2, 1) + one(3, 1), self_parts(4, 0), cross_parts(0), one(9, 0) + one(10, 0),
                    self_parts(4, 1) + cross_parts(1), one(9, 1) + one(10, 1)]
        *packs, x_row = run_pack(sources_a[:4] + [x_enc], groups_a, row=4)
        packs += list(run_pack(sources_b, groups_b))
        x_row = permute('x', x_row)
        w = [spread(pack) for pack in packs]

        full_lead, mid_lead = (0, 2), (1, 0)
        same = [(0, 0)]

        def job(full, tq, tks, h, plans=(None,), **extra):
            return dict(full=full, tq=tq, tks=tks, h=h, plans=plans, **extra)

        def flat(*slots_sizes):
            return [(slot, None, size, same) for slot, size in slots_sizes]

        hs, ht = src // 2, tgt // 2
        x_mid = [(0, mid_lead, hs, [(0, 1), (1, -1)])]
        y_mid = [(0, mid_lead, CHUNK, [(0, 1), (3, -1), (1, -1), (2, 1)])]
        y_full = [(0, full_lead, tgt, same)]
        e_own, d_own, c_own = (enc_qkv_t, enc_wo), (dec_qkv_t, dec_wo), (crs_wq, crs_kv_t, crs_wo)

        def self_phase(**kwargs):
            return dict(cross=False, gain=0, **kwargs)

        def cross_phase(**kwargs):
            return dict(cross=True, gain=1, own=c_own, **kwargs)

        mid_plan, full_plan = (MID_CHUNKS, None), (FULL_CHUNKS, None)
        pd_mid, pd_full = run_block(own_len, dec_norm, 0, [self_phase(own=d_own)],
                                [job(False, ht, (tgt,), y_mid, mid_plan), job(True, tgt, (tgt,), y_full, full_plan)], [y_dec], part_out=True)
        pe_mid, pe_full = run_block(own_len, enc_norm, 0, [self_phase(own=e_own)],
                                [job(False, hs, (src,), x_mid), job(True, src, (src,), flat((1, src)))], [x_enc, x_row], part_out=True)
        h_mid, h_full = run_block(own_len, enc_norm, 0, [self_phase(pieces=w[0])],
                              [job(False, hs, (src,), x_mid, part=flat((2, hs))), job(True, src, (src,), flat((1, src)), part=flat((3, src)))],
                              [x_enc, x_row, pe_mid, pe_full], part_in=True)
        h_mid, h_full = run_block(own_len, enc_norm, 0, [], [job(False, hs, (), flat((0, hs))), job(True, src, (), flat((1, src)))],
                              [h_mid, h_full], ff_gain=1, ff=(enc_w1, enc_w2, w[1], w[1]), down_base=D)
        h_other = permute('y', h_mid)
        e1 = dict(ff_gain=1, ff=(enc_w1, enc_w2, w[3], w[3]), down_base=D, final_gain=enc_final)
        e1_phases = [self_phase(own=e_own, pieces=w[2])]
        s_full, = run_block(own_len, enc_norm, 1, e1_phases, [job(True, src, (src,), flat((0, src)))], [h_full], **e1)
        s_mid, = run_block(own_len, enc_norm, 1, e1_phases, [job(False, hs, (src,), flat((0, hs), (1, hs)))], [h_mid, h_other], **e1)
        s_mid = permute('x', s_mid)
        s_other = permute('y', s_mid)

        z_mid, = run_block(own_len, dec_norm, 0, [self_phase(pieces=w[4])],
                       [job(False, ht, (tgt,), y_mid, mid_plan, part=flat((1, ht)))], [y_dec, pd_mid], part_in=True)
        cross0, cross1 = cross_phase(pieces=w[5]), cross_phase(pieces=w[7], base=D)
        ff0 = dict(ff_gain=2, ff=(dec_w1, dec_w2, w[6], w[6]), down_base=D)
        ff1 = dict(ff_gain=2, ff=(dec_w1, dec_w2, w[8], w[8]), down_base=D)
        z_full, = run_block(own_len, dec_norm, 0, [self_phase(pieces=w[4]), cross0],
                        [job(True, tgt, (tgt, src), y_full, full_plan, part=flat((1, tgt)), src=flat((2, src)))], [y_dec, pd_full, s_full],
                        part_in=True, **ff0)
        z_mid, = run_block(own_len, dec_norm, 0, [cross0], [job(False, ht, (src,), flat((0, ht)), src=flat((1, hs), (2, hs)))],
                       [z_mid, s_mid, s_other], **ff0)
        z_other = permute('y', z_mid)
        d1_phases = [self_phase(own=d_own, pieces=w[7]), cross1]
        z_full, = run_block(own_len, dec_norm, 1, d1_phases, [job(True, tgt, (tgt, src), flat((0, tgt)), full_plan, src=flat((1, src)))],
                        [z_full, s_full], **ff1)
        z_full_other = permute('y', z_full)
        z_mid, = run_block(own_len, dec_norm, 1, d1_phases,
                       [job(False, ht, (tgt, src), flat((0, ht), (1, ht)), mid_plan, src=flat((2, hs), (3, hs)))],
                       [z_mid, z_other, s_mid, s_other], **ff1)
        z_mid_other = permute('y', z_mid)

        first = lax.axis_index('model') == 0
        a, b, oa, ob = z_mid[:CHUNK], z_mid[CHUNK:], z_mid_other[:CHUNK], z_mid_other[CHUNK:]
        row_mid = jnp.where(first, jnp.concatenate([a, oa, ob, b], axis=0), jnp.concatenate([oa, a, b, ob], axis=0))
        rows = jnp.stack([jnp.where(first, z_full, z_full_other), z_full, jnp.where(first, z_full_other, z_full)])
        return lax.dynamic_update_slice_in_dim(lax.optimization_barrier(rows), row_mid[None], 1, 0)

    return jax.shard_map(local_step, mesh=mesh, in_specs=in_specs_all, out_specs=row_spec, check_vma=False)
```
